256 devices in a mesh: time: 64 (over z_lo, y, x, core), chan: 4 (over z_hi).
Axes of the slice: x: 4, y: 4, z: 8 (z_hi: 4, z_lo: 2; z = z_hi * 2 + z_lo), core: 2. Of those that a mesh axis runs over, the one named last changes fastest.
Arguments:
- decay_rate: float32 [4, 32768, 2560], P(None, 'time', 'chan'), may hold values from 0.2 to 2
- drive_in: bfloat16 [4, 32768, 2560], P(None, 'time', 'chan'), may hold values from -6 to 6
- gate_in: bfloat16 [4, 32768, 2560], P(None, 'time', 'chan'), may hold values from -6 to 6
- norm_gain: float32 [2560], P('chan'), may hold values from 0.25 to 1.75
Outputs:
- filtered: bfloat16 [4, 32768, 2560], P(None, 'time', 'chan')
The draws below stay inside these ranges and needn't reach their ends.
All inputs are finite; a program needn't handle non-finite values.
Results may differ from the reference program's by a relative error of at most 0.0015.
Values sent between devices are 32-bit elements.
A program may use at most 128 MiB of HBM per device.

```python
import jax
import jax.numpy as jnp
from jax import lax

BATCH = 4
CHANNELS = 2560
LENGTH = 32768


def levels(rng, extent, cuts, least, largest):
    level = 1.0
    for position, shards_of in cuts:
        steps = jax.random.uniform(jax.random.fold_in(jax.random.fold_in(rng, 6), position), (shards_of,), jnp.float32, least / len(cuts), largest / len(cuts))
        level = level * jnp.repeat(jnp.exp(steps), extent[position] // shards_of).reshape((-1,) + (1,) * (len(extent) - 1 - position))
    return level


def bell_draw(key, dims, scale, limit, pieces=(), kind=jnp.bfloat16):
    array = scale * jax.random.normal(key, dims, jnp.float32)
    if pieces:
        array = array * levels(key, dims, pieces, -0.22, 0.18)
    return jnp.clip(array, -limit, limit).astype(kind)


def setup_inputs(seed: int = 0) -> dict:
    arg_keys = jax.random.split(jax.random.key(seed), 5)
    return {
        "decay_rate": jnp.clip(0.2 + 1.8 * jax.random.uniform(arg_keys[0], (BATCH, LENGTH, CHANNELS), jnp.float32) ** levels(arg_keys[0], (BATCH, LENGTH, CHANNELS), ((1, 64), (2, 4)), -0.2, 0.2), 0.2, 2.0),
        "drive_in": bell_draw(arg_keys[1], (BATCH, LENGTH, CHANNELS), 1.0, 6.0, ((1, 64), (2, 4))),
        "gate_in": bell_draw(arg_keys[2], (BATCH, LENGTH, CHANNELS), 1.0, 6.0, ((1, 64), (2, 4))),
        "norm_gain": jnp.clip(1.0 + 0.15 * jax.random.normal(arg_keys[3], (CHANNELS,), jnp.float32), 0.25, 1.75),
    }


def join_pair(earlier, later):
    return (earlier[0] * later[0], later[0] * earlier[1] + later[1])

def reference(decay_rate, drive_in, gate_in, norm_gain):
    keep = jnp.exp(-decay_rate / LENGTH)
    push = drive_in.astype(jnp.float32) * LENGTH ** (-0.5)
    forward = lax.associative_scan(join_pair, (keep, push), axis=1)[1]
    gated = forward * jax.nn.sigmoid(gate_in.astype(jnp.float32))
    power = lax.optimization_barrier(jnp.mean(gated * gated, axis=-1, keepdims=True))
    filtered = (gated * lax.rsqrt(power + 1e-06) * norm_gain).astype(jnp.bfloat16)
    return filtered
```

```python
import functools
import math

import jax
import jax.numpy as jnp
from jax import lax
from jax.experimental import pallas as pl
from jax.experimental.pallas import tpu as pltpu
from jax.sharding import PartitionSpec as P

MESH = pl.DeviceIdType.MESH
BLOCK = 256
LANES = 128
CHUNK = 16
COLS = 8
F32 = jnp.float32
BF16 = jnp.bfloat16
NT = (((1,), (1,)), ((), ()))
TN = (((0,), (0,)), ((), ()))


def iota(shape, dim):
    return lax.broadcasted_iota(jnp.int32, shape, dim)


def triangle(width):
    row, column = iota((BLOCK, width), 0), iota((BLOCK, width), 1)
    return jnp.where(lax.rem(column, BLOCK) <= row, 1.0, 0.0).astype(BF16)


def by_rows(x):
    return x.reshape(x.shape[0] // 8, 8, x.shape[1]).sum(0)


def state_kernel(
    times, chans, decay_hbm, drive_hbm, gate_hbm, gated_ref, scale_ref,
    decay, drives, gate, logs, local, squares, ends, row_buf, col_buf, power_buf,
    decay_sem, drive_sem, gate_sem, row_send, row_recv, col_send, col_recv, power_send, power_recv,
):
    batch, length, width = decay_hbm.shape
    halves = length // BLOCK
    blocks = batch * halves
    rows = times // COLS
    total_length = length * times
    log2_scale = math.log2(math.e) / total_length
    time, chan = lax.axis_index("time"), lax.axis_index("chan")
    row, col = time // COLS, lax.rem(time, COLS)

    def at(ref, block):
        return ref.at[block // halves, pl.ds(block % halves * BLOCK, BLOCK), :]

    loads = {}
    for block in range(blocks):
        loads["decay", block] = pltpu.make_async_copy(at(decay_hbm, block), decay.at[block], decay_sem.at[block])
        loads["drive", block] = pltpu.make_async_copy(at(drive_hbm, block), drives.at[block, 0], drive_sem.at[block])
        loads["gate", block] = pltpu.make_async_copy(at(gate_hbm, block), gate.at[block], gate_sem.at[block])
    for block in range(blocks):
        loads["decay", block].start()
        loads["drive", block].start()
    for block in range(blocks):
        loads["gate", block].start()

    row_peers = [(row * COLS + lax.rem(col + k, COLS), chan) for k in range(1, COLS)]
    col_peers = [(lax.rem(row + k, rows) * COLS + col, chan) for k in range(1, rows)]
    chan_peers = [(time, lax.rem(chan + k, chans)) for k in range(1, chans)]
    barrier = pltpu.get_barrier_semaphore()
    for peer in row_peers + col_peers + chan_peers:
        pl.semaphore_signal(barrier, inc=1, device_id=peer, device_id_type=MESH)

    lower = triangle(BLOCK)
    both = triangle(2 * BLOCK)

    for block in range(blocks):
        loads["decay", block].wait()
        logs[block] = jnp.dot(lower, decay[block].astype(BF16), preferred_element_type=F32)
        loads["drive", block].wait()

        def step(i, carry):
            drive_sum, decay_sum = carry
            here = pl.ds(pl.multiple_of(i * CHUNK, CHUNK), CHUNK)
            drive = drives[block, 0, here, :].astype(F32)
            grown = drive * jnp.exp2(logs[block, here, :] * log2_scale)
            drives[block, 1, here, :] = (grown - drive).astype(BF16)
            return drive_sum + by_rows(grown), decay_sum + by_rows(decay[block, here, :])

        zero = jnp.zeros((8, width), F32)
        drive_sum, decay_sum = lax.fori_loop(0, BLOCK // CHUNK, step, (zero, zero), unroll=2)
        shrink = jnp.exp2(decay_sum.sum(0, keepdims=True) * -log2_scale)
        ends[block : block + 1, :] = shrink
        ends[blocks + block : blocks + block + 1, :] = shrink * drive_sum.sum(0, keepdims=True)

    for b in range(batch):
        keep, state = jnp.ones((1, width), F32), jnp.zeros((1, width), F32)
        for block in range(b * halves, (b + 1) * halves):
            shrink = ends[block : block + 1, :]
            keep, state = keep * shrink, shrink * state + ends[blocks + block : blocks + block + 1, :]
        row_buf[col, b : b + 1, :] = keep
        row_buf[col, batch + b : batch + b + 1, :] = state

    pl.semaphore_wait(barrier, len(row_peers + col_peers + chan_peers))
    row_copies = [
        pltpu.make_async_remote_copy(
            row_buf.at[col], row_buf.at[col], row_send.at[k], row_recv.at[col], device_id=peer, device_id_type=MESH
        )
        for k, peer in enumerate(row_peers)
    ]
    for copy in row_copies:
        copy.start()

    def gate_block(block):
        stacked = drives[block].reshape(2 * BLOCK, width)
        local[block] = jnp.dot(both, stacked, preferred_element_type=F32)
        loads["gate", block].wait()

        def step(i, carry):
            here = pl.ds(pl.multiple_of(i * CHUNK, CHUNK), CHUNK)
            half = 0.5 * total_length**-0.5
            sigmoid = jnp.tanh(gate[block, here, :].astype(F32) * 0.5) * half + half
            logs[block, here, :] = jnp.exp2(logs[block, here, :] * -log2_scale) * sigmoid
            return carry

        lax.fori_loop(0, BLOCK // CHUNK, step, 0, unroll=2)

    for block in range(blocks // 2):
        gate_block(block)

    for k in range(1, COLS):
        source = lax.rem(col + k, COLS)
        pltpu.make_async_remote_copy(
            row_buf.at[source], row_buf.at[source], row_send.at[k - 1], row_recv.at[source],
            device_id=(time, chan), device_id_type=MESH,
        ).wait_recv()
    keep, state = jnp.ones((batch, width), F32), jnp.zeros((batch, width), F32)
    keep_before, state_before = keep, state
    for j in range(COLS):
        a, b = row_buf[j, :batch, :], row_buf[j, batch:, :]
        keep, state = a * keep, a * state + b
        passed = j < col
        keep_before, state_before = jnp.where(passed, keep, keep_before), jnp.where(passed, state, state_before)
    col_buf[row, :batch, :] = keep
    col_buf[row, batch:, :] = state
    col_copies = []
    for k in range(1, rows):
        copy = pltpu.make_async_remote_copy(
            col_buf.at[row], col_buf.at[row], col_send.at[k - 1], col_recv.at[row],
            device_id=(lax.rem(row + k, rows) * COLS + col, chan), device_id_type=MESH,
        )
        col_copies.append(copy)
        pl.when(row + k < rows)(copy.start)

    for block in range(blocks // 2, blocks):
        gate_block(block)

    for k in range(1, rows):
        source = lax.rem(row + k, rows)
        copy = pltpu.make_async_remote_copy(
            col_buf.at[source], col_buf.at[source], col_send.at[k - 1], col_recv.at[source],
            device_id=(time, chan), device_id_type=MESH,
        )
        pl.when(source < row)(copy.wait_recv)
    entering = jnp.zeros((batch, width), F32)
    for j in range(rows):
        new = col_buf[j, :batch, :] * entering + col_buf[j, batch:, :]
        entering = jnp.where(j < row, new, entering)
    entering = keep_before * entering + state_before

    powers = jnp.zeros((blocks, BLOCK), F32)
    for b in range(batch):
        start = entering[b : b + 1, :]
        for block in range(b * halves, (b + 1) * halves):
            where = block % halves * BLOCK

            def step(i, carry):
                here = pl.ds(pl.multiple_of(i * CHUNK, CHUNK), CHUNK)
                there = pl.ds(pl.multiple_of(where + i * CHUNK, CHUNK), CHUNK)
                gated = logs[block, here, :] * (local[block, here, :] + start)
                gated_ref[b, there, :] = gated
                square = gated * gated
                squares[here, :] = sum(square[:, k : k + LANES] for k in range(0, width, LANES))
                return carry

            lax.fori_loop(0, BLOCK // CHUNK, step, 0, unroll=2)
            high = squares[...].astype(BF16)
            rest = (squares[...] - high.astype(F32)).astype(BF16)
            pick = jnp.where(iota((blocks, 2 * LANES), 0) == block, 1.0, 0.0).astype(BF16)
            powers = powers + lax.dot_general(
                pick, jnp.concatenate([high, rest], axis=1), NT, preferred_element_type=F32
            )
            if block + 1 < (b + 1) * halves:
                start = ends[block : block + 1, :] * (local[block, BLOCK - 1 :, :] + start)
    power_buf[chan] = powers
    power_copies = [
        pltpu.make_async_remote_copy(
            power_buf.at[chan], power_buf.at[chan], power_send.at[k], power_recv.at[chan],
            device_id=peer, device_id_type=MESH,
        )
        for k, peer in enumerate(chan_peers)
    ]
    for copy in power_copies:
        copy.start()
    for k in range(1, chans):
        source = lax.rem(chan + k, chans)
        pltpu.make_async_remote_copy(
            power_buf.at[source], power_buf.at[source], power_send.at[k - 1], power_recv.at[source],
            device_id=(time, chan), device_id_type=MESH,
        ).wait_recv()
    power = sum(power_buf[j] for j in range(chans)) / (width * chans)
    scale_ref[...] = lax.rsqrt(power + 1e-06)

    for copy in row_copies + power_copies:
        copy.wait_send()
    for k, copy in enumerate(col_copies):
        pl.when(row + k + 1 < rows)(copy.wait_send)


def scale_kernel(gated_ref, scale_ref, gain_ref, out_ref):
    block = pl.program_id(0) * pl.num_programs(1) + pl.program_id(1)
    blocks = scale_ref.shape[0]
    pick = jnp.where(iota((blocks, LANES), 0) == block, 1.0, 0.0)
    scale = lax.dot_general(scale_ref[...], pick, TN, precision=lax.Precision.HIGHEST, preferred_element_type=F32)
    for k in range(0, out_ref.shape[-1], LANES):
        lane = slice(k, k + LANES)
        out_ref[0, :, lane] = (gated_ref[0, :, lane] * scale * gain_ref[:, lane]).astype(out_ref.dtype)


def solution(mesh):
    times, chans = mesh.shape["time"], mesh.shape["chan"]

    def body(decay_rate, drive_in, gate_in, norm_gain):
        batch, length, width = decay_rate.shape
        halves = length // BLOCK
        blocks = batch * halves
        rows = times // COLS
        dma = pltpu.SemaphoreType.DMA
        gated, scale = pl.pallas_call(
            functools.partial(state_kernel, times, chans),
            out_shape=(pltpu.VMEM((batch, length, width), F32), pltpu.VMEM((blocks, BLOCK), F32)),
            in_specs=[pl.BlockSpec(memory_space=pltpu.HBM)] * 3,
            out_specs=(pl.BlockSpec(memory_space=pltpu.VMEM), pl.BlockSpec(memory_space=pltpu.VMEM)),
            scratch_shapes=[
                pltpu.VMEM((blocks, BLOCK, width), F32),
                pltpu.VMEM((blocks, 2, BLOCK, width), BF16),
                pltpu.VMEM((blocks, BLOCK, width), BF16),
                pltpu.VMEM((blocks, BLOCK, width), F32),
                pltpu.VMEM((blocks, BLOCK, width), F32),
                pltpu.VMEM((BLOCK, LANES), F32),
                pltpu.VMEM((2 * blocks, width), F32),
                pltpu.VMEM((COLS, 2 * batch, width), F32),
                pltpu.VMEM((rows, 2 * batch, width), F32),
                pltpu.VMEM((chans, blocks, BLOCK), F32),
                dma((blocks,)), dma((blocks,)), dma((blocks,)),
                dma((COLS - 1,)), dma((COLS,)),
                dma((rows - 1,)), dma((rows,)),
                dma((chans - 1,)), dma((chans,)),
            ],
            compiler_params=pltpu.CompilerParams(
                collective_id=0, has_side_effects=True, vmem_limit_bytes=40 * 2**20
            ),
        )(decay_rate, drive_in, gate_in)
        return pl.pallas_call(
            scale_kernel,
            out_shape=jax.ShapeDtypeStruct((batch, length, width), BF16),
            grid=(batch, halves),
            in_specs=[
                pl.BlockSpec((1, BLOCK, width), lambda b, h: (b, h, 0)),
                pl.BlockSpec((blocks, BLOCK), lambda b, h: (0, 0)),
                pl.BlockSpec((1, width), lambda b, h: (0, 0)),
            ],
            out_specs=pl.BlockSpec((1, BLOCK, width), lambda b, h: (b, h, 0)),
            compiler_params=pltpu.CompilerParams(vmem_limit_bytes=16 * 2**20),
        )(gated, scale, norm_gain.reshape(1, width))

    in_specs = (P(None, "time", "chan"), P(None, "time", "chan"), P(None, "time", "chan"), P("chan"))
    return jax.shard_map(body, mesh=mesh, in_specs=in_specs, out_specs=P(None, "time", "chan"), check_vma=False)
```

```python
import functools
import math

import jax
import jax.numpy as jnp
from jax import lax
from jax.experimental import pallas as pl
from jax.experimental.pallas import tpu as pltpu
from jax.sharding import PartitionSpec as P

MESH = pl.DeviceIdType.MESH
BLOCK = 256
LANES = 128
CHUNK = 16
COLS = 8
F32 = jnp.float32
BF16 = jnp.bfloat16
NT = (((1,), (1,)), ((), ()))
TN = (((0,), (0,)), ((), ()))


def iota(shape, dim):
    return lax.broadcasted_iota(jnp.int32, shape, dim)


def triangle(width):
    row, column = iota((BLOCK, width), 0), iota((BLOCK, width), 1)
    return jnp.where(lax.rem(column, BLOCK) <= row, 1.0, 0.0).astype(BF16)


def by_rows(x):
    return x.reshape(x.shape[0] // 8, 8, x.shape[1]).sum(0)


def state_kernel(
    times, chans, decay_hbm, drive_hbm, gate_hbm, gated_ref, scale_ref,
    decay, drives, gate, logs, local, squares, ends, row_buf, col_buf, power_buf,
    decay_sem, drive_sem, gate_sem, row_send, row_recv, col_send, col_recv, power_send, power_recv,
):
    batch, length, width = decay_hbm.shape
    halves = length // BLOCK
    blocks = batch * halves
    rows = times // COLS
    total_length = length * times
    log2_scale = math.log2(math.e) / total_length
    time, chan = lax.axis_index("time"), lax.axis_index("chan")
    row, col = time // COLS, lax.rem(time, COLS)

    def at(ref, block):
        return ref.at[block // halves, pl.ds(block % halves * BLOCK, BLOCK), :]

    loads = {}
    for block in range(blocks):
        loads["decay", block] = pltpu.make_async_copy(at(decay_hbm, block), decay.at[block], decay_sem.at[block])
        loads["drive", block] = pltpu.make_async_copy(at(drive_hbm, block), drives.at[block, 0], drive_sem.at[block])
        loads["gate", block] = pltpu.make_async_copy(at(gate_hbm, block), gate.at[block], gate_sem.at[block])
    for block in range(blocks):
        loads["decay", block].start()
        loads["drive", block].start()
    for block in range(blocks):
        loads["gate", block].start()

    row_peers = [(row * COLS + lax.rem(col + k, COLS), chan) for k in range(1, COLS)]
    col_peers = [(lax.rem(row + k, rows) * COLS + col, chan) for k in range(1, rows)]
    chan_peers = [(time, lax.rem(chan + k, chans)) for k in range(1, chans)]
    barrier = pltpu.get_barrier_semaphore()
    for peer in row_peers + col_peers + chan_peers:
        pl.semaphore_signal(barrier, inc=1, device_id=peer, device_id_type=MESH)

    lower = triangle(BLOCK)
    both = triangle(2 * BLOCK)

    for block in range(blocks):
        loads["decay", block].wait()
        logs[block] = jnp.dot(lower, decay[block].astype(BF16), preferred_element_type=F32)
        loads["drive", block].wait()

        def step(i, carry):
            drive_sum, decay_sum = carry
            here = pl.ds(pl.multiple_of(i * CHUNK, CHUNK), CHUNK)
            drive = drives[block, 0, here, :].astype(F32)
            grown = drive * jnp.exp2(logs[block, here, :] * log2_scale)
            drives[block, 1, here, :] = (grown - drive).astype(BF16)
            return drive_sum + by_rows(grown), decay_sum + by_rows(decay[block, here, :])

        zero = jnp.zeros((8, width), F32)
        drive_sum, decay_sum = lax.fori_loop(0, BLOCK // CHUNK, step, (zero, zero), unroll=2)
        shrink = jnp.exp2(decay_sum.sum(0, keepdims=True) * -log2_scale)
        ends[block : block + 1, :] = shrink
        ends[blocks + block : blocks + block + 1, :] = shrink * drive_sum.sum(0, keepdims=True)

    for b in range(batch):
        keep, state = jnp.ones((1, width), F32), jnp.zeros((1, width), F32)
        for block in range(b * halves, (b + 1) * halves):
            shrink = ends[block : block + 1, :]
            keep, state = keep * shrink, shrink * state + ends[blocks + block : blocks + block + 1, :]
        row_buf[col, b : b + 1, :] = keep
        row_buf[col, batch + b : batch + b + 1, :] = state

    pl.semaphore_wait(barrier, len(row_peers + col_peers + chan_peers))
    row_copies = [
        pltpu.make_async_remote_copy(
            row_buf.at[col], row_buf.at[col], row_send.at[k], row_recv.at[col], device_id=peer, device_id_type=MESH
        )
        for k, peer in enumerate(row_peers)
    ]
    for copy in row_copies:
        copy.start()

    def gate_block(block):
        stacked = drives[block].reshape(2 * BLOCK, width)
        local[block] = jnp.dot(both, stacked, preferred_element_type=F32)
        loads["gate", block].wait()

        def step(i, carry):
            here = pl.ds(pl.multiple_of(i * CHUNK, CHUNK), CHUNK)
            half = 0.5 * total_length**-0.5
            sigmoid = jnp.tanh(gate[block, here, :].astype(F32) * 0.5) * half + half
            logs[block, here, :] = jnp.exp2(logs[block, here, :] * -log2_scale) * sigmoid
            return carry

        lax.fori_loop(0, BLOCK // CHUNK, step, 0, unroll=2)

    for block in range(blocks // 2):
        gate_block(block)

    for k in range(1, COLS):
        source = lax.rem(col + k, COLS)
        pltpu.make_async_remote_copy(
            row_buf.at[source], row_buf.at[source], row_send.at[k - 1], row_recv.at[source],
            device_id=(time, chan), device_id_type=MESH,
        ).wait_recv()
    keep, state = jnp.ones((batch, width), F32), jnp.zeros((batch, width), F32)
    keep_before, state_before = keep, state
    for j in range(COLS):
        a, b = row_buf[j, :batch, :], row_buf[j, batch:, :]
        keep, state = a * keep, a * state + b
        passed = j < col
        keep_before, state_before = jnp.where(passed, keep, keep_before), jnp.where(passed, state, state_before)
    col_buf[row, :batch, :] = keep
    col_buf[row, batch:, :] = state
    col_copies = []
    for k in range(1, rows):
        copy = pltpu.make_async_remote_copy(
            col_buf.at[row], col_buf.at[row], col_send.at[k - 1], col_recv.at[row],
            device_id=(lax.rem(row + k, rows) * COLS + col, chan), device_id_type=MESH,
        )
        col_copies.append(copy)
        pl.when(row + k < rows)(copy.start)

    for block in range(blocks // 2, blocks):
        gate_block(block)

    for k in range(1, rows):
        source = lax.rem(row + k, rows)
        copy = pltpu.make_async_remote_copy(
            col_buf.at[source], col_buf.at[source], col_send.at[k - 1], col_recv.at[source],
            device_id=(time, chan), device_id_type=MESH,
        )
        pl.when(source < row)(copy.wait_recv)
    entering = jnp.zeros((batch, width), F32)
    for j in range(rows):
        new = col_buf[j, :batch, :] * entering + col_buf[j, batch:, :]
        entering = jnp.where(j < row, new, entering)
    entering = keep_before * entering + state_before

    powers = jnp.zeros((blocks, BLOCK), F32)
    for b in range(batch):
        start = entering[b : b + 1, :]
        for block in range(b * halves, (b + 1) * halves):
            where = block % halves * BLOCK

            def step(i, carry):
                here = pl.ds(pl.multiple_of(i * CHUNK, CHUNK), CHUNK)
                there = pl.ds(pl.multiple_of(where + i * CHUNK, CHUNK), CHUNK)
                gated = logs[block, here, :] * (local[block, here, :] + start)
                gated_ref[b, there, :] = gated
                square = gated * gated
                squares[here, :] = sum(square[:, k : k + LANES] for k in range(0, width, LANES))
                return carry

            lax.fori_loop(0, BLOCK // CHUNK, step, 0, unroll=2)
            high = squares[...].astype(BF16)
            rest = (squares[...] - high.astype(F32)).astype(BF16)
            pick = jnp.where(iota((blocks, 2 * LANES), 0) == block, 1.0, 0.0).astype(BF16)
            powers = powers + lax.dot_general(
                pick, jnp.concatenate([high, rest], axis=1), NT, preferred_element_type=F32
            )
            if block + 1 < (b + 1) * halves:
                start = ends[block : block + 1, :] * (local[block, BLOCK - 1 :, :] + start)
    power_buf[chan] = powers
    power_copies = [
        pltpu.make_async_remote_copy(
            power_buf.at[chan], power_buf.at[chan], power_send.at[k], power_recv.at[chan],
            device_id=peer, device_id_type=MESH,
        )
        for k, peer in enumerate(chan_peers)
    ]
    for copy in power_copies:
        copy.start()
    for k in range(1, chans):
        source = lax.rem(chan + k, chans)
        pltpu.make_async_remote_copy(
            power_buf.at[source], power_buf.at[source], power_send.at[k - 1], power_recv.at[source],
            device_id=(time, chan), device_id_type=MESH,
        ).wait_recv()
    power = sum(power_buf[j] for j in range(chans)) / (width * chans)
    scale_ref[...] = lax.rsqrt(power + 1e-06)

    for copy in row_copies + power_copies:
        copy.wait_send()
    for k, copy in enumerate(col_copies):
        pl.when(row + k + 1 < rows)(copy.wait_send)


def scale_kernel(gated_ref, scale_ref, gain_ref, out_ref):
    block = pl.program_id(0) * pl.num_programs(1) + pl.program_id(1)
    scale = scale_ref[pl.ds(block, 1), :]
    high = scale.astype(BF16)
    rest = (scale - high.astype(F32)).astype(BF16)
    square = (BLOCK, BLOCK)
    diagonal = iota(square, 0) == iota(square, 1)
    spread = [jnp.where(diagonal, jnp.broadcast_to(part.astype(F32), square), 0.0).astype(BF16) for part in (high, rest)]
    ones = jnp.ones((2 * BLOCK, LANES), BF16)
    scale = jnp.dot(jnp.concatenate(spread, axis=1), ones, preferred_element_type=F32)
    for k in range(0, out_ref.shape[-1], LANES):
        lane = slice(k, k + LANES)
        gain = gain_ref[lane].reshape(1, LANES)
        out_ref[0, :, lane] = (gated_ref[0, :, lane] * scale * gain).astype(out_ref.dtype)


def solution(mesh):
    times, chans = mesh.shape["time"], mesh.shape["chan"]

    def body(decay_rate, drive_in, gate_in, norm_gain):
        batch, length, width = decay_rate.shape
        halves = length // BLOCK
        blocks = batch * halves
        rows = times // COLS
        dma = pltpu.SemaphoreType.DMA
        gated, scale = pl.pallas_call(
            functools.partial(state_kernel, times, chans),
            out_shape=(pltpu.VMEM((batch, length, width), F32), pltpu.VMEM((blocks, BLOCK), F32)),
            in_specs=[pl.BlockSpec(memory_space=pltpu.HBM)] * 3,
            out_specs=(pl.BlockSpec(memory_space=pltpu.VMEM), pl.BlockSpec(memory_space=pltpu.VMEM)),
            scratch_shapes=[
                pltpu.VMEM((blocks, BLOCK, width), F32),
                pltpu.VMEM((blocks, 2, BLOCK, width), BF16),
                pltpu.VMEM((blocks, BLOCK, width), BF16),
                pltpu.VMEM((blocks, BLOCK, width), F32),
                pltpu.VMEM((blocks, BLOCK, width), F32),
                pltpu.VMEM((BLOCK, LANES), F32),
                pltpu.VMEM((2 * blocks, width), F32),
                pltpu.VMEM((COLS, 2 * batch, width), F32),
                pltpu.VMEM((rows, 2 * batch, width), F32),
                pltpu.VMEM((chans, blocks, BLOCK), F32),
                dma((blocks,)), dma((blocks,)), dma((blocks,)),
                dma((COLS - 1,)), dma((COLS,)),
                dma((rows - 1,)), dma((rows,)),
                dma((chans - 1,)), dma((chans,)),
            ],
            compiler_params=pltpu.CompilerParams(
                collective_id=0, has_side_effects=True, vmem_limit_bytes=57 * 2**20
            ),
        )(decay_rate, drive_in, gate_in)
        return pl.pallas_call(
            scale_kernel,
            out_shape=jax.ShapeDtypeStruct((batch, length, width), BF16),
            grid=(batch, halves),
            in_specs=[
                pl.BlockSpec((1, BLOCK, width), lambda b, h: (b, h, 0)),
                pl.BlockSpec((blocks, BLOCK), lambda b, h: (0, 0)),
                pl.BlockSpec((width,), lambda b, h: (0,)),
            ],
            out_specs=pl.BlockSpec((1, BLOCK, width), lambda b, h: (b, h, 0)),
            compiler_params=pltpu.CompilerParams(vmem_limit_bytes=16 * 2**20),
        )(gated, scale, norm_gain)

    in_specs = (P(None, "time", "chan"), P(None, "time", "chan"), P(None, "time", "chan"), P("chan"))
    return jax.shard_map(body, mesh=mesh, in_specs=in_specs, out_specs=P(None, "time", "chan"), check_vma=False)
```

```python
import functools
import math

import jax
import jax.numpy as jnp
from jax import lax
from jax.experimental import pallas as pl
from jax.experimental.pallas import tpu as pltpu
from jax.sharding import PartitionSpec as P

MESH = pl.DeviceIdType.MESH
BLOCK = 256
LANES = 128
CHUNK = 16
COLS = 8
F32 = jnp.float32
BF16 = jnp.bfloat16
NT = (((1,), (1,)), ((), ()))
TN = (((0,), (0,)), ((), ()))


def iota(shape, dim):
    return lax.broadcasted_iota(jnp.int32, shape, dim)


def triangle(width):
    row, column = iota((BLOCK, width), 0), iota((BLOCK, width), 1)
    return jnp.where(lax.rem(column, BLOCK) <= row, 1.0, 0.0).astype(BF16)


def parts(x):
    high = x.astype(BF16)
    return high, (x - high.astype(F32)).astype(BF16)


def state_kernel(
    times, chans, decay_hbm, drive_hbm, gate_hbm, gated_ref, scale_ref,
    decay, drives, gate, logs, local, rounded, lower, ends, row_buf, col_buf, power_buf,
    decay_sem, drive_sem, row_send, row_recv, col_send, col_recv, power_send, power_recv,
):
    batch, length, width = decay_hbm.shape
    halves = length // BLOCK
    blocks = batch * halves
    rows = times // COLS
    total_length = length * times
    log2_scale = math.log2(math.e) / total_length
    time, chan = lax.axis_index("time"), lax.axis_index("chan")
    row, col = time // COLS, lax.rem(time, COLS)

    def at(ref, block):
        return ref.at[block // halves, pl.ds(block % halves * BLOCK, BLOCK), :]

    decays = [pltpu.make_async_copy(at(decay_hbm, k), decay.at[k], decay_sem.at[k]) for k in range(blocks)]
    driving = [pltpu.make_async_copy(at(drive_hbm, k), drives.at[k, 0], drive_sem.at[k]) for k in range(blocks)]
    gates = [pltpu.make_async_copy(at(gate_hbm, k), gate.at[k], decay_sem.at[k]) for k in range(blocks)]
    for k in range(blocks):
        decays[k].start()
        driving[k].start()

    row_peers = [(row * COLS + lax.rem(col + k, COLS), chan) for k in range(1, COLS)]
    col_peers = [(lax.rem(row + k, rows) * COLS + col, chan) for k in range(1, rows)]
    chan_peers = [(time, lax.rem(chan + k, chans)) for k in range(1, chans)]
    peers = row_peers + col_peers + chan_peers
    barrier = pltpu.get_barrier_semaphore()
    for peer in peers:
        pl.semaphore_signal(barrier, inc=1, device_id=peer, device_id_type=MESH)

    lower[...] = triangle(2 * BLOCK)
    chunks = [slice(k, k + CHUNK) for k in range(0, BLOCK, CHUNK)]

    def cumulate(block):
        decays[block].wait()
        total = jnp.zeros((8, width), F32)
        for here in chunks:
            rate = decay[block, here, :]
            total = total + (rate[:8] + rate[8:])
            rounded[block % 2, here, :] = rate.astype(BF16)
        ends[block : block + 1, :] = jnp.exp2(total.sum(0, keepdims=True) * -log2_scale)
        logs[block] = jnp.dot(lower[:, :BLOCK], rounded[block % 2], preferred_element_type=F32)

    def grow(block):
        driving[block].wait()
        total = jnp.zeros((8, width), F32)
        for here in chunks:
            drive = drives[block, 0, here, :].astype(F32)
            grown = drive * jnp.exp2(logs[block, here, :] * log2_scale)
            total = total + (grown[:8] + grown[8:])
            drives[block, 1, here, :] = (grown - drive).astype(BF16)
        ends[blocks + block : blocks + block + 1, :] = ends[block : block + 1, :] * total.sum(0, keepdims=True)

    def send_row(which):
        for peer in row_peers:
            pltpu.make_async_remote_copy(
                row_buf.at[which, col], row_buf.at[which, col], row_send, row_recv.at[which],
                device_id=peer, device_id_type=MESH,
            ).start()

    def wait_row(which):
        several = row_buf.at[which, pl.ds(0, COLS - 1)]
        pltpu.make_async_copy(several, several, row_recv.at[which]).wait()

    def col_copy(which, k, source):
        return pltpu.make_async_remote_copy(
            col_buf.at[source, which], col_buf.at[source, which], col_send.at[k], col_recv.at[source],
            device_id=col_peers[k], device_id_type=MESH,
        )

    def send_col(which):
        for k in range(rows - 1):
            pl.when(row + k + 1 < rows)(col_copy(which, k, row).start)

    cumulate(0)
    for block in range(blocks):
        if block + 1 < blocks:
            cumulate(block + 1)
        if block + 2 == blocks:
            for b in range(batch):
                first = b * halves
                row_buf[0, col, b : b + 1, :] = functools.reduce(
                    jnp.multiply, [ends[first + k : first + k + 1, :] for k in range(halves)]
                )
            pl.semaphore_wait(barrier, len(peers))
            send_row(0)
        if block >= blocks // 2:
            for k in range(2 * (block - blocks // 2), 2 * (block - blocks // 2) + 2):
                gates[k].start()
        grow(block)

    for b in range(batch):
        first = b * halves
        state = ends[blocks + first : blocks + first + 1, :]
        for k in range(first + 1, first + halves):
            state = ends[k : k + 1, :] * state + ends[blocks + k : blocks + k + 1, :]
        row_buf[1, col, b : b + 1, :] = state
    send_row(1)

    def gate_block(block):
        gates[block].wait()
        local[block] = jnp.dot(lower[...], drives[block].reshape(2 * BLOCK, width), preferred_element_type=F32)
        for here in chunks:
            half = 0.5 * total_length**-0.5
            sigmoid = jnp.tanh(gate[block, here, :].astype(F32) * 0.5) * half + half
            logs[block, here, :] = jnp.exp2(logs[block, here, :] * -log2_scale) * sigmoid

    for block in range(blocks // 2):
        gate_block(block)

    wait_row(0)
    keep_before, keep = jnp.ones((batch, width), F32), jnp.ones((batch, width), F32)
    for j in range(COLS):
        keep = row_buf[0, j] * keep
        keep_before = jnp.where(j < col, keep, keep_before)
    col_buf[row, 0] = keep
    send_col(0)
    gate_block(blocks // 2)

    wait_row(1)
    state = state_before = jnp.zeros((batch, width), F32)
    for j in range(COLS):
        state = row_buf[0, j] * state + row_buf[1, j]
        state_before = jnp.where(j < col, state, state_before)
    col_buf[row, 1] = state
    send_col(1)

    for block in range(blocks // 2 + 1, blocks):
        gate_block(block)

    for k in range(1, rows):
        source = lax.rem(row + k, rows)
        copy = pltpu.make_async_copy(col_buf.at[source], col_buf.at[source], col_recv.at[source])
        pl.when(source < row)(copy.wait)
    entering = jnp.zeros((batch, width), F32)
    for j in range(rows):
        entering = jnp.where(j < row, col_buf[j, 0] * entering + col_buf[j, 1], entering)
    entering = keep_before * entering + state_before

    powers = jnp.zeros((blocks, BLOCK), F32)
    for b in range(batch):
        start = entering[b : b + 1, :]
        for block in range(b * halves, (b + 1) * halves):
            where = block % halves * BLOCK
            squares = []
            for here in chunks:
                gated = logs[block, here, :] * (local[block, here, :] + start)
                gated_ref[b, where + here.start : where + here.stop, :] = gated
                square = gated * gated
                square = sum(square[:, k : k + LANES] for k in range(0, width, LANES))
                squares.append(jnp.concatenate(parts(square), axis=1))
            pick = jnp.where(iota((blocks, 2 * LANES), 0) == block, 1.0, 0.0).astype(BF16)
            powers = powers + lax.dot_general(
                pick, jnp.concatenate(squares, axis=0), NT, preferred_element_type=F32
            )
            if block + 1 < (b + 1) * halves:
                start = ends[block : block + 1, :] * (local[block, BLOCK - 1 :, :] + start)
    power_buf[chan] = powers
    for peer in chan_peers:
        pltpu.make_async_remote_copy(
            power_buf.at[chan], power_buf.at[chan], power_send, power_recv, device_id=peer, device_id_type=MESH
        ).start()
    several = power_buf.at[pl.ds(0, chans - 1)]
    pltpu.make_async_copy(several, several, power_recv).wait()
    power = sum(power_buf[j] for j in range(chans)) / (width * chans)
    scale_ref[...] = lax.rsqrt(power + 1e-06)

    for which in range(2):
        several = row_buf.at[which, pl.ds(0, COLS - 1)]
        pltpu.make_async_copy(several, several, row_send).wait()
    for k in range(rows - 1):
        pl.when(row + k + 1 < rows)(pltpu.make_async_copy(col_buf.at[row], col_buf.at[row], col_send.at[k]).wait)
    several = power_buf.at[pl.ds(0, chans - 1)]
    pltpu.make_async_copy(several, several, power_send).wait()


def scale_kernel(gated_ref, scale_ref, gain_ref, out_hbm, result, factors, sem):
    batch, length, width = result.shape
    blocks = scale_ref.shape[0]
    halves = blocks // batch
    wide = (2 * blocks, blocks * LANES)
    pick = jnp.where(lax.rem(iota(wide, 0), blocks) == iota(wide, 1) // LANES, 1.0, 0.0).astype(BF16)
    factors[...] = lax.dot_general(
        jnp.concatenate(parts(scale_ref[...]), axis=0), pick, TN, preferred_element_type=F32
    )
    gain = gain_ref[...].reshape(1, width)
    for block in range(blocks):
        b, where = block // halves, block % halves * BLOCK
        for k in range(0, BLOCK, CHUNK):
            here = slice(where + k, where + k + CHUNK)
            factor = factors[k : k + CHUNK, block * LANES : (block + 1) * LANES]
            factor = jnp.concatenate([factor] * (width // LANES), axis=1)
            result[b, here, :] = (gated_ref[b, here, :] * factor * gain).astype(result.dtype)
        there = (b, pl.ds(where, BLOCK))
        pltpu.make_async_copy(result.at[there], out_hbm.at[there], sem).start()
    pltpu.make_async_copy(result, out_hbm, sem).wait()


def solution(mesh):
    times, chans = mesh.shape["time"], mesh.shape["chan"]

    def body(decay_rate, drive_in, gate_in, norm_gain):
        batch, length, width = decay_rate.shape
        blocks = batch * length // BLOCK
        rows = times // COLS
        dma = pltpu.SemaphoreType.DMA
        vmem = pl.BlockSpec(memory_space=pltpu.VMEM)
        gated, scale = pl.pallas_call(
            functools.partial(state_kernel, times, chans),
            out_shape=(pltpu.VMEM((batch, length, width), F32), pltpu.VMEM((blocks, BLOCK), F32)),
            in_specs=[pl.BlockSpec(memory_space=pltpu.HBM)] * 3,
            out_specs=(vmem, vmem),
            scratch_shapes=[
                pltpu.VMEM((blocks, BLOCK, width), F32),
                pltpu.VMEM((blocks, 2, BLOCK, width), BF16),
                pltpu.VMEM((blocks, BLOCK, width), BF16),
                pltpu.VMEM((blocks, BLOCK, width), F32),
                pltpu.VMEM((blocks, BLOCK, width), F32),
                pltpu.VMEM((2, BLOCK, width), BF16),
                pltpu.VMEM((BLOCK, 2 * BLOCK), BF16),
                pltpu.VMEM((2 * blocks, width), F32),
                pltpu.VMEM((2, COLS, batch, width), F32),
                pltpu.VMEM((rows, 2, batch, width), F32),
                pltpu.VMEM((chans, blocks, BLOCK), F32),
                dma((blocks,)), dma((blocks,)),
                dma, dma((2,)),
                dma((rows - 1,)), dma((rows,)),
                dma, dma,
            ],
            compiler_params=pltpu.CompilerParams(
                collective_id=0, has_side_effects=True, vmem_limit_bytes=57 * 2**20
            ),
        )(decay_rate, drive_in, gate_in)
        return pl.pallas_call(
            scale_kernel,
            out_shape=jax.ShapeDtypeStruct((batch, length, width), BF16),
            in_specs=[vmem, vmem, vmem],
            out_specs=pl.BlockSpec(memory_space=pltpu.HBM),
            scratch_shapes=[
                pltpu.VMEM((batch, length, width), BF16),
                pltpu.VMEM((BLOCK, blocks * LANES), F32),
                dma,
            ],
            compiler_params=pltpu.CompilerParams(vmem_limit_bytes=16 * 2**20),
        )(gated, scale, norm_gain)

    in_specs = (P(None, "time", "chan"), P(None, "time", "chan"), P(None, "time", "chan"), P("chan"))
    return jax.shard_map(body, mesh=mesh, in_specs=in_specs, out_specs=P(None, "time", "chan"), check_vma=False)
```

```python
import functools
import math

import jax
import jax.numpy as jnp
from jax import lax
from jax.experimental import pallas as pl
from jax.experimental.pallas import tpu as pltpu
from jax.sharding import PartitionSpec as P

MESH = pl.DeviceIdType.MESH
BLOCK = 256
LANES = 128
CHUNK = 16
COLS = 8
F32 = jnp.float32
BF16 = jnp.bfloat16
NT = (((1,), (1,)), ((), ()))
TN = (((0,), (0,)), ((), ()))


def iota(shape, dim):
    return lax.broadcasted_iota(jnp.int32, shape, dim)


def triangle(width):
    row, column = iota((BLOCK, width), 0), iota((BLOCK, width), 1)
    return jnp.where(lax.rem(column, BLOCK) <= row, 1.0, 0.0).astype(BF16)


def parts(x):
    high = x.astype(BF16)
    return high, (x - high.astype(F32)).astype(BF16)


def state_kernel(
    times, chans, decay_hbm, drive_hbm, gate_hbm, gated_ref, scale_ref,
    decay, drives, gate, logs, local, rounded, lower, ends, row_buf, col_buf, power_buf,
    decay_sem, drive_sem, row_send, row_recv, col_send, col_recv, power_send, power_recv,
):
    batch, length, width = decay_hbm.shape
    halves = length // BLOCK
    blocks = batch * halves
    rows = times // COLS
    total_length = length * times
    log2_scale = math.log2(math.e) / total_length
    time, chan = lax.axis_index("time"), lax.axis_index("chan")
    row, col = time // COLS, lax.rem(time, COLS)

    def at(ref, block):
        return ref.at[block // halves, pl.ds(block % halves * BLOCK, BLOCK), :]

    decays = [pltpu.make_async_copy(at(decay_hbm, k), decay.at[k], decay_sem.at[k]) for k in range(blocks)]
    driving = [pltpu.make_async_copy(at(drive_hbm, k), drives.at[k, 0], drive_sem.at[k]) for k in range(blocks)]
    gates = [pltpu.make_async_copy(at(gate_hbm, k), gate.at[k], decay_sem.at[k]) for k in range(blocks)]
    for k in range(blocks):
        decays[k].start()
        driving[k].start()

    row_peers = [(row * COLS + lax.rem(col + k, COLS), chan) for k in range(1, COLS)]
    col_peers = [(lax.rem(row + k, rows) * COLS + col, chan) for k in range(1, rows)]
    chan_peers = [(time, lax.rem(chan + k, chans)) for k in range(1, chans)]
    peers = row_peers + col_peers + chan_peers
    barrier = pltpu.get_barrier_semaphore()
    for peer in peers:
        pl.semaphore_signal(barrier, inc=1, device_id=peer, device_id_type=MESH)

    lower[...] = triangle(2 * BLOCK)
    chunks = [slice(k, k + CHUNK) for k in range(0, BLOCK, CHUNK)]
    none = jnp.zeros((1, width), F32)
    one = jnp.ones((1, width), F32)

    def cumulate(block):
        total = jnp.zeros((8, width), F32)
        for here in chunks:
            rate = decay[block, here, :]
            total = total + (rate[:8] + rate[8:])
            rounded[block % 2, here, :] = rate.astype(BF16)
        ends[block : block + 1, :] = jnp.exp2(total.sum(0, keepdims=True) * -log2_scale)
        logs[block] = jnp.dot(lower[:, :BLOCK], rounded[block % 2], preferred_element_type=F32)

    def grow(block):
        total = jnp.zeros((8, width), F32)
        for here in chunks:
            drive = drives[block, 0, here, :].astype(F32)
            grown = drive * jnp.exp2(logs[block, here, :] * log2_scale)
            total = total + (grown[:8] + grown[8:])
            drives[block, 1, here, :] = (grown - drive).astype(BF16)
        ends[blocks + block : blocks + block + 1, :] = ends[block : block + 1, :] * total.sum(0, keepdims=True)

    def send_row(b):
        keep, state = one, none
        for k in range(b * halves, (b + 1) * halves):
            shrink = ends[k : k + 1, :]
            keep, state = shrink * keep, shrink * state + ends[blocks + k : blocks + k + 1, :]
        row_buf[col, b, 0:1, :] = keep
        row_buf[col, b, 1:2, :] = state
        if b == 0:
            pl.semaphore_wait(barrier, len(peers))
        for peer in row_peers:
            pltpu.make_async_remote_copy(
                row_buf.at[col, b], row_buf.at[col, b], row_send, row_recv.at[b],
                device_id=peer, device_id_type=MESH,
            ).start()

    before = {}

    def send_col(b):
        several = row_buf.at[pl.ds(0, COLS - 1), b]
        pltpu.make_async_copy(several, several, row_recv.at[b]).wait()
        keep, state = one, none
        keep_before, state_before = keep, state
        for j in range(COLS):
            keep, state = row_buf[j, b, 0:1, :] * keep, row_buf[j, b, 0:1, :] * state + row_buf[j, b, 1:2, :]
            keep_before, state_before = jnp.where(j < col, keep, keep_before), jnp.where(j < col, state, state_before)
        before[b] = keep_before, state_before
        col_buf[row, b, 0:1, :] = keep
        col_buf[row, b, 1:2, :] = state
        for k in range(rows - 1):
            copy = pltpu.make_async_remote_copy(
                col_buf.at[row, b], col_buf.at[row, b], col_send.at[k], col_recv.at[b, row],
                device_id=col_peers[k], device_id_type=MESH,
            )
            pl.when(row + k + 1 < rows)(copy.start)

    def enter(b):
        for k in range(1, rows):
            source = lax.rem(row + k, rows)
            copy = pltpu.make_async_copy(col_buf.at[source, b], col_buf.at[source, b], col_recv.at[b, source])
            pl.when(source < row)(copy.wait)
        state = none
        for j in range(rows):
            state = jnp.where(j < row, col_buf[j, b, 0:1, :] * state + col_buf[j, b, 1:2, :], state)
        keep_before, state_before = before[b]
        return keep_before * state + state_before

    def gate_block(block):
        local[block] = jnp.dot(lower[...], drives[block].reshape(2 * BLOCK, width), preferred_element_type=F32)
        for here in chunks:
            half = 0.5 * total_length**-0.5
            sigmoid = jnp.tanh(gate[block, here, :].astype(F32) * 0.5) * half + half
            logs[block, here, :] = jnp.exp2(logs[block, here, :] * -log2_scale) * sigmoid

    def gate_batch(b):
        for block in range(b * halves, (b + 1) * halves):
            gates[block].wait()
        for block in range(b * halves, (b + 1) * halves):
            gate_block(block)

    def finish(b):
        start = enter(b)
        powers = jnp.zeros((halves, BLOCK), F32)
        for half in range(halves):
            block, where = b * halves + half, half * BLOCK
            squares = []
            for here in chunks:
                gated = logs[block, here, :] * (local[block, here, :] + start)
                gated_ref[b, where + here.start : where + here.stop, :] = gated
                square = gated * gated
                square = sum(square[:, k : k + LANES] for k in range(0, width, LANES))
                squares.append(jnp.concatenate(parts(square), axis=1))
            pick = jnp.where(iota((halves, 2 * LANES), 0) == half, 1.0, 0.0).astype(BF16)
            powers = powers + lax.dot_general(
                pick, jnp.concatenate(squares, axis=0), NT, preferred_element_type=F32
            )
            if half + 1 < halves:
                start = ends[block : block + 1, :] * (local[block, BLOCK - 1 :, :] + start)
        power_buf[chan, b] = powers
        for peer in chan_peers:
            pltpu.make_async_remote_copy(
                power_buf.at[chan, b], power_buf.at[chan, b], power_send, power_recv,
                device_id=peer, device_id_type=MESH,
            ).start()

    decays[0].wait()
    cumulate(0)
    for block in range(blocks):
        if block + 1 < blocks:
            decays[block + 1].wait()
        driving[block].wait()
        if block == blocks // 2:
            for copy in gates[:blocks // 2]:
                copy.start()
        if block + 1 < blocks:
            cumulate(block + 1)
        grow(block)
        if block % halves == halves - 1:
            send_row(block // halves)
    for copy in gates[blocks // 2 :]:
        copy.start()

    gate_batch(0)
    gate_batch(1)
    send_col(0)
    for b in range(2, batch):
        gate_batch(b)
        send_col(b - 1)
    send_col(batch - 1)
    for b in range(batch):
        finish(b)

    several = power_buf.at[pl.ds(0, chans - 1)]
    pltpu.make_async_copy(several, several, power_recv).wait()
    for b in range(batch):
        power = sum(power_buf[j, b] for j in range(chans)) / (width * chans)
        scale_ref[b * halves : (b + 1) * halves, :] = lax.rsqrt(power + 1e-06)

    several = row_buf.at[pl.ds(0, COLS - 1)]
    pltpu.make_async_copy(several, several, row_send).wait()
    for k in range(rows - 1):
        pl.when(row + k + 1 < rows)(pltpu.make_async_copy(col_buf.at[row], col_buf.at[row], col_send.at[k]).wait)
    several = power_buf.at[pl.ds(0, chans - 1)]
    pltpu.make_async_copy(several, several, power_send).wait()


def scale_kernel(gated_ref, scale_ref, gain_ref, out_hbm, result, factors, sem):
    batch, length, width = result.shape
    blocks = scale_ref.shape[0]
    halves = blocks // batch
    wide = (2 * blocks, blocks * LANES)
    pick = jnp.where(lax.rem(iota(wide, 0), blocks) == iota(wide, 1) // LANES, 1.0, 0.0).astype(BF16)
    factors[...] = lax.dot_general(
        jnp.concatenate(parts(scale_ref[...]), axis=0), pick, TN, preferred_element_type=F32
    )
    gain = gain_ref[...].reshape(1, width)
    for block in range(blocks):
        b, where = block // halves, block % halves * BLOCK
        for k in range(0, BLOCK, CHUNK):
            here = slice(where + k, where + k + CHUNK)
            factor = factors[k : k + CHUNK, block * LANES : (block + 1) * LANES]
            factor = jnp.concatenate([factor] * (width // LANES), axis=1)
            result[b, here, :] = (gated_ref[b, here, :] * factor * gain).astype(result.dtype)
        there = (b, pl.ds(where, BLOCK))
        pltpu.make_async_copy(result.at[there], out_hbm.at[there], sem).start()
    pltpu.make_async_copy(result, out_hbm, sem).wait()


def solution(mesh):
    times, chans = mesh.shape["time"], mesh.shape["chan"]

    def body(decay_rate, drive_in, gate_in, norm_gain):
        batch, length, width = decay_rate.shape
        blocks = batch * length // BLOCK
        rows = times // COLS
        dma = pltpu.SemaphoreType.DMA
        vmem = pl.BlockSpec(memory_space=pltpu.VMEM)
        gated, scale = pl.pallas_call(
            functools.partial(state_kernel, times, chans),
            out_shape=(pltpu.VMEM((batch, length, width), F32), pltpu.VMEM((blocks, BLOCK), F32)),
            in_specs=[pl.BlockSpec(memory_space=pltpu.HBM)] * 3,
            out_specs=(vmem, vmem),
            scratch_shapes=[
                pltpu.VMEM((blocks, BLOCK, width), F32),
                pltpu.VMEM((blocks, 2, BLOCK, width), BF16),
                pltpu.VMEM((blocks, BLOCK, width), BF16),
                pltpu.VMEM((blocks, BLOCK, width), F32),
                pltpu.VMEM((blocks, BLOCK, width), F32),
                pltpu.VMEM((2, BLOCK, width), BF16),
                pltpu.VMEM((BLOCK, 2 * BLOCK), BF16),
                pltpu.VMEM((2 * blocks, width), F32),
                pltpu.VMEM((COLS, batch, 2, width), F32),
                pltpu.VMEM((rows, batch, 2, width), F32),
                pltpu.VMEM((chans, batch, length // BLOCK, BLOCK), F32),
                dma((blocks,)), dma((blocks,)),
                dma, dma((batch,)),
                dma((rows - 1,)), dma((batch, rows)),
                dma, dma,
            ],
            compiler_params=pltpu.CompilerParams(
                collective_id=0, has_side_effects=True, vmem_limit_bytes=57 * 2**20
            ),
        )(decay_rate, drive_in, gate_in)
        return pl.pallas_call(
            scale_kernel,
            out_shape=jax.ShapeDtypeStruct((batch, length, width), BF16),
            in_specs=[vmem, vmem, vmem],
            out_specs=pl.BlockSpec(memory_space=pltpu.HBM),
            scratch_shapes=[
                pltpu.VMEM((batch, length, width), BF16),
                pltpu.VMEM((BLOCK, blocks * LANES), F32),
                dma,
            ],
            compiler_params=pltpu.CompilerParams(vmem_limit_bytes=16 * 2**20),
        )(gated, scale, norm_gain)

    in_specs = (P(None, "time", "chan"), P(None, "time", "chan"), P(None, "time", "chan"), P("chan"))
    return jax.shard_map(body, mesh=mesh, in_specs=in_specs, out_specs=P(None, "time", "chan"), check_vma=False)
```

```python
import functools
import math

import jax
import jax.numpy as jnp
from jax import lax
from jax.experimental import pallas as pl
from jax.experimental.pallas import tpu as pltpu
from jax.sharding import PartitionSpec as P

MESH = pl.DeviceIdType.MESH
BLOCK = 256
LANES = 128
CHUNK = 16
COLS = 8
F32 = jnp.float32
BF16 = jnp.bfloat16
NT = (((1,), (1,)), ((), ()))
TN = (((0,), (0,)), ((), ()))


def iota(shape, dim):
    return lax.broadcasted_iota(jnp.int32, shape, dim)


def triangle(width, value):
    row, column = iota((BLOCK, width), 0), iota((BLOCK, width), 1)
    return jnp.where(lax.rem(column, BLOCK) <= row, value, 0.0).astype(BF16)


def parts(x):
    high = x.astype(BF16)
    return high, (x - high.astype(F32)).astype(BF16)


def state_kernel(
    times, chans, decay_hbm, drive_hbm, gate_hbm, gated_ref, scale_ref,
    decay, drives, gate, logs, local, rounded, fall, lower, ends, row_buf, col_buf, power_buf,
    decay_sem, drive_sem, row_send, row_recv, col_send, col_recv, power_send, power_recv,
):
    batch, length, width = decay_hbm.shape
    halves = length // BLOCK
    blocks = batch * halves
    rows = times // COLS
    total_length = length * times
    log2_scale = math.log2(math.e) / total_length
    half = 0.5 * total_length**-0.5
    time, chan = lax.axis_index("time"), lax.axis_index("chan")
    row, col = time // COLS, lax.rem(time, COLS)

    def at(ref, block):
        return ref.at[block // halves, pl.ds(block % halves * BLOCK, BLOCK), :]

    decays = [pltpu.make_async_copy(at(decay_hbm, k), decay.at[k], decay_sem.at[k]) for k in range(blocks)]
    driving = [pltpu.make_async_copy(at(drive_hbm, k), drives.at[k, 0], drive_sem.at[k]) for k in range(blocks)]
    gates = [pltpu.make_async_copy(at(gate_hbm, k), gate.at[k], decay_sem.at[k]) for k in range(blocks)]
    decays[0].start()
    for k in range(blocks):
        if k + 1 < blocks:
            decays[k + 1].start()
        driving[k].start()

    row_peers = [(row * COLS + lax.rem(col + k, COLS), chan) for k in range(1, COLS)]
    col_peers = [(lax.rem(row + k, rows) * COLS + col, chan) for k in range(1, rows)]
    chan_peers = [(time, lax.rem(chan + k, chans)) for k in range(1, chans)]
    peers = row_peers + col_peers + chan_peers
    barrier = pltpu.get_barrier_semaphore()
    for peer in peers:
        pl.semaphore_signal(barrier, inc=1, device_id=peer, device_id_type=MESH)

    fall[...] = triangle(BLOCK, -log2_scale)
    lower[...] = triangle(2 * BLOCK, 1.0)
    chunks = [slice(k, k + CHUNK) for k in range(0, BLOCK, CHUNK)]
    none = jnp.zeros((1, width), F32)
    one = jnp.ones((1, width), F32)

    def prepare(block):
        total = jnp.zeros((8, width), F32)
        for here in chunks:
            rate = decay[block, here, :]
            total = total + (rate[:8] + rate[8:])
            rounded[block % 2, here, :] = rate.astype(BF16)
        ends[block : block + 1, :] = jnp.exp2(total.sum(0, keepdims=True) * -log2_scale)

    def grow(block):
        fallen = jnp.dot(fall[...], rounded[block % 2], preferred_element_type=F32)
        total = jnp.zeros((8, width), F32)
        for here in chunks:
            logs[block, here, :] = fallen[here]
            drive = drives[block, 0, here, :].astype(F32)
            added = drive * (jnp.exp2(-fallen[here]) - 1.0)
            drives[block, 1, here, :] = added.astype(BF16)
            added = added + drive
            total = total + (added[:8] + added[8:])
        ends[blocks + block : blocks + block + 1, :] = ends[block : block + 1, :] * total.sum(0, keepdims=True)

    def send_row(b):
        keep, state = one, none
        for k in range(b * halves, (b + 1) * halves):
            shrink = ends[k : k + 1, :]
            keep, state = shrink * keep, shrink * state + ends[blocks + k : blocks + k + 1, :]
        row_buf[col, b, 0:1, :] = keep
        row_buf[col, b, 1:2, :] = state

    def start_row(b):
        for peer in row_peers:
            pltpu.make_async_remote_copy(
                row_buf.at[col, b], row_buf.at[col, b], row_send, row_recv.at[b],
                device_id=peer, device_id_type=MESH,
            ).start()

    before = {}

    def send_col(b):
        several = row_buf.at[pl.ds(0, COLS - 1), b]
        pltpu.make_async_copy(several, several, row_recv.at[b]).wait()
        keep, state = one, none
        keep_before, state_before = keep, state
        for j in range(COLS):
            keep, state = row_buf[j, b, 0:1, :] * keep, row_buf[j, b, 0:1, :] * state + row_buf[j, b, 1:2, :]
            keep_before, state_before = jnp.where(j < col, keep, keep_before), jnp.where(j < col, state, state_before)
        before[b] = keep_before, state_before
        col_buf[row, b, 0:1, :] = keep
        col_buf[row, b, 1:2, :] = state
        for k in range(rows - 1):
            copy = pltpu.make_async_remote_copy(
                col_buf.at[row, b], col_buf.at[row, b], col_send, col_recv.at[b],
                device_id=col_peers[k], device_id_type=MESH,
            )
            pl.when(row + k + 1 < rows)(copy.start)

    def enter(b):
        for k in range(1, rows):
            several = col_buf.at[pl.ds(0, k), b]
            pl.when(row == k)(pltpu.make_async_copy(several, several, col_recv.at[b]).wait)
        state = none
        for j in range(rows):
            state = jnp.where(j < row, col_buf[j, b, 0:1, :] * state + col_buf[j, b, 1:2, :], state)
        keep_before, state_before = before[b]
        return keep_before * state + state_before

    def gate_block(block):
        local[block] = jnp.dot(lower[...], drives[block].reshape(2 * BLOCK, width), preferred_element_type=F32)
        for here in chunks:
            opening = jnp.tanh((gate[block, here, :] * 0.5).astype(F32)) + 1.0
            logs[block, here, :] = jnp.exp2(logs[block, here, :]) * opening

    def gate_batch(b):
        for block in range(b * halves, (b + 1) * halves):
            gates[block].wait()
        for block in range(b * halves, (b + 1) * halves):
            gate_block(block)

    def finish(b):
        start = enter(b)
        powers = jnp.zeros((halves, BLOCK), F32)
        for part in range(halves):
            block, where = b * halves + part, part * BLOCK
            squares = []
            for here in chunks:
                gated = logs[block, here, :] * (local[block, here, :] + start)
                gated_ref[b, where + here.start : where + here.stop, :] = gated
                square = gated * gated
                square = sum(square[:, k : k + LANES] for k in range(0, width, LANES))
                squares.append(jnp.concatenate(parts(square), axis=1))
            pick = jnp.where(iota((halves, 2 * LANES), 0) == part, 1.0, 0.0).astype(BF16)
            powers = powers + lax.dot_general(
                pick, jnp.concatenate(squares, axis=0), NT, preferred_element_type=F32
            )
            if part + 1 < halves:
                start = ends[block : block + 1, :] * (local[block, BLOCK - 1 :, :] + start)
        power_buf[chan, b] = powers
        for peer in chan_peers:
            pltpu.make_async_remote_copy(
                power_buf.at[chan, b], power_buf.at[chan, b], power_send, power_recv,
                device_id=peer, device_id_type=MESH,
            ).start()

    decays[0].wait()
    prepare(0)
    for block in range(blocks):
        if block + 1 < blocks:
            decays[block + 1].wait()
        driving[block].wait()
        if block == blocks // 2:
            for copy in gates[:blocks // 2]:
                copy.start()
        grow(block)
        if block + 1 < blocks:
            prepare(block + 1)
        if block % halves == halves - 1 and block + 1 < blocks:
            send_row(block // halves)
            if block + 1 + halves == blocks:
                pl.semaphore_wait(barrier, len(peers))
                for b in range(batch - 1):
                    start_row(b)
    send_row(batch - 1)
    start_row(batch - 1)
    for copy in gates[blocks // 2 :]:
        copy.start()

    gate_batch(0)
    gate_batch(1)
    send_col(0)
    for b in range(2, batch):
        gate_batch(b)
        send_col(b - 1)
    send_col(batch - 1)
    for b in range(batch):
        finish(b)

    several = power_buf.at[pl.ds(0, chans - 1)]
    pltpu.make_async_copy(several, several, power_recv).wait()
    for b in range(batch):
        power = sum(power_buf[j, b] for j in range(chans)) * (half * half / (width * chans))
        scale_ref[b * halves : (b + 1) * halves, :] = half * lax.rsqrt(power + 1e-06)

    several = row_buf.at[pl.ds(0, COLS - 1)]
    pltpu.make_async_copy(several, several, row_send).wait()
    for k in range(1, rows):
        several = col_buf.at[pl.ds(0, k)]
        pl.when(row + k + 1 == rows)(pltpu.make_async_copy(several, several, col_send).wait)
    several = power_buf.at[pl.ds(0, chans - 1)]
    pltpu.make_async_copy(several, several, power_send).wait()


def scale_kernel(gated_ref, scale_ref, gain_ref, out_hbm, result, factors, sem):
    batch, length, width = result.shape
    blocks = scale_ref.shape[0]
    halves = blocks // batch
    wide = (2 * blocks, blocks * LANES)
    pick = jnp.where(lax.rem(iota(wide, 0), blocks) == iota(wide, 1) // LANES, 1.0, 0.0).astype(BF16)
    factors[...] = lax.dot_general(
        jnp.concatenate(parts(scale_ref[...]), axis=0), pick, TN, preferred_element_type=F32
    )
    gain = gain_ref[...].reshape(1, width)
    for block in range(blocks):
        b, where = block // halves, block % halves * BLOCK
        for k in range(0, BLOCK, CHUNK):
            here = slice(where + k, where + k + CHUNK)
            factor = factors[k : k + CHUNK, block * LANES : (block + 1) * LANES]
            factor = jnp.concatenate([factor] * (width // LANES), axis=1)
            result[b, here, :] = (gated_ref[b, here, :] * factor * gain).astype(result.dtype)
        there = (b, pl.ds(where, BLOCK))
        pltpu.make_async_copy(result.at[there], out_hbm.at[there], sem).start()
    pltpu.make_async_copy(result, out_hbm, sem).wait()


def solution(mesh):
    times, chans = mesh.shape["time"], mesh.shape["chan"]

    def body(decay_rate, drive_in, gate_in, norm_gain):
        batch, length, width = decay_rate.shape
        blocks = batch * length // BLOCK
        rows = times // COLS
        dma = pltpu.SemaphoreType.DMA
        vmem = pl.BlockSpec(memory_space=pltpu.VMEM)
        gated, scale = pl.pallas_call(
            functools.partial(state_kernel, times, chans),
            out_shape=(pltpu.VMEM((batch, length, width), F32), pltpu.VMEM((blocks, BLOCK), F32)),
            in_specs=[pl.BlockSpec(memory_space=pltpu.HBM)] * 3,
            out_specs=(vmem, vmem),
            scratch_shapes=[
                pltpu.VMEM((blocks, BLOCK, width), F32),
                pltpu.VMEM((blocks, 2, BLOCK, width), BF16),
                pltpu.VMEM((blocks, BLOCK, width), BF16),
                pltpu.VMEM((blocks, BLOCK, width), F32),
                pltpu.VMEM((blocks, BLOCK, width), F32),
                pltpu.VMEM((2, BLOCK, width), BF16),
                pltpu.VMEM((BLOCK, BLOCK), BF16),
                pltpu.VMEM((BLOCK, 2 * BLOCK), BF16),
                pltpu.VMEM((2 * blocks, width), F32),
                pltpu.VMEM((COLS, batch, 2, width), F32),
                pltpu.VMEM((rows, batch, 2, width), F32),
                pltpu.VMEM((chans, batch, length // BLOCK, BLOCK), F32),
                dma((blocks,)), dma((blocks,)),
                dma, dma((batch,)),
                dma, dma((batch,)),
                dma, dma,
            ],
            compiler_params=pltpu.CompilerParams(
                collective_id=0, has_side_effects=True, vmem_limit_bytes=57 * 2**20
            ),
        )(decay_rate, drive_in, gate_in)
        return pl.pallas_call(
            scale_kernel,
            out_shape=jax.ShapeDtypeStruct((batch, length, width), BF16),
            in_specs=[vmem, vmem, vmem],
            out_specs=pl.BlockSpec(memory_space=pltpu.HBM),
            scratch_shapes=[
                pltpu.VMEM((batch, length, width), BF16),
                pltpu.VMEM((BLOCK, blocks * LANES), F32),
                dma,
            ],
            compiler_params=pltpu.CompilerParams(vmem_limit_bytes=16 * 2**20),
        )(gated, scale, norm_gain)

    in_specs = (P(None, "time", "chan"), P(None, "time", "chan"), P(None, "time", "chan"), P("chan"))
    return jax.shard_map(body, mesh=mesh, in_specs=in_specs, out_specs=P(None, "time", "chan"), check_vma=False)
```

```python
import functools
import math

import jax
import jax.numpy as jnp
from jax import lax
from jax.experimental import pallas as pl
from jax.experimental.pallas import tpu as pltpu
from jax.sharding import PartitionSpec as P

MESH = pl.DeviceIdType.MESH
BLOCK = 256
LANES = 128
CHUNK = 16
COLS = 8
F32 = jnp.float32
BF16 = jnp.bfloat16
NT = (((1,), (1,)), ((), ()))
TN = (((0,), (0,)), ((), ()))


def iota(shape, dim):
    return lax.broadcasted_iota(jnp.int32, shape, dim)


def triangle(width, value):
    row, column = iota((BLOCK, width), 0), iota((BLOCK, width), 1)
    return jnp.where(lax.rem(column, BLOCK) <= row, value, 0.0).astype(BF16)


def parts(x):
    high = x.astype(BF16)
    return high, (x - high.astype(F32)).astype(BF16)


def state_kernel(
    times, chans, decay_hbm, drive_hbm, gate_hbm, gated_ref, scale_ref,
    decay, drives, gate, logs, local, rounded, fall, lower, ends, row_buf, col_buf, power_buf,
    decay_sem, drive_sem, row_send, row_recv, col_send, col_recv, power_send, power_recv,
):
    batch, length, width = decay_hbm.shape
    halves = length // BLOCK
    blocks = batch * halves
    rows = times // COLS
    total_length = length * times
    log2_scale = math.log2(math.e) / total_length
    half = 0.5 * total_length**-0.5
    time, chan = lax.axis_index("time"), lax.axis_index("chan")
    row, col = time // COLS, lax.rem(time, COLS)

    def at(ref, block):
        return ref.at[block // halves, pl.ds(block % halves * BLOCK, BLOCK), :]

    decays = [pltpu.make_async_copy(at(decay_hbm, k), decay.at[k], decay_sem.at[k]) for k in range(blocks)]
    driving = [pltpu.make_async_copy(at(drive_hbm, k), drives.at[k, 0], drive_sem.at[k]) for k in range(blocks)]
    gates = [pltpu.make_async_copy(at(gate_hbm, k), gate.at[k], decay_sem.at[k]) for k in range(blocks)]
    decays[0].start()
    for k in range(blocks):
        if k + 1 < blocks:
            decays[k + 1].start()
        driving[k].start()

    row_peers = [(row * COLS + lax.rem(col + k, COLS), chan) for k in range(1, COLS)]
    col_peers = [(lax.rem(row + k, rows) * COLS + col, chan) for k in range(1, rows)]
    chan_peers = [(time, lax.rem(chan + k, chans)) for k in range(1, chans)]
    peers = row_peers + col_peers + chan_peers
    barrier = pltpu.get_barrier_semaphore()
    for peer in peers:
        pl.semaphore_signal(barrier, inc=1, device_id=peer, device_id_type=MESH)

    fall[...] = triangle(BLOCK, -log2_scale)
    lower[...] = triangle(2 * BLOCK, 1.0)
    chunks = [slice(k, k + CHUNK) for k in range(0, BLOCK, CHUNK)]
    none = jnp.zeros((1, width), F32)
    one = jnp.ones((1, width), F32)

    def prepare(block):
        total = jnp.zeros((8, width), F32)
        for here in chunks:
            rate = decay[block, here, :]
            total = total + (rate[:8] + rate[8:])
            rounded[block % 2, here, :] = rate.astype(BF16)
        ends[block : block + 1, :] = jnp.exp2(total.sum(0, keepdims=True) * -log2_scale)

    def grow(block):
        fallen = jnp.dot(fall[...], rounded[block % 2], preferred_element_type=F32)
        total = jnp.zeros((8, width), F32)
        for here in chunks:
            logs[block, here, :] = fallen[here]
            drive = drives[block, 0, here, :].astype(F32)
            added = drive * (jnp.exp2(-fallen[here]) - 1.0)
            drives[block, 1, here, :] = added.astype(BF16)
            added = added + drive
            total = total + (added[:8] + added[8:])
        ends[blocks + block : blocks + block + 1, :] = ends[block : block + 1, :] * total.sum(0, keepdims=True)

    def send_row(b):
        keep, state = one, none
        for k in range(b * halves, (b + 1) * halves):
            shrink = ends[k : k + 1, :]
            keep, state = shrink * keep, shrink * state + ends[blocks + k : blocks + k + 1, :]
        row_buf[col, b, 0:1, :] = keep
        row_buf[col, b, 1:2, :] = state

    def start_row(b):
        for peer in row_peers:
            pltpu.make_async_remote_copy(
                row_buf.at[col, b], row_buf.at[col, b], row_send, row_recv.at[b],
                device_id=peer, device_id_type=MESH,
            ).start()

    before = {}

    def send_col(b):
        several = row_buf.at[pl.ds(0, COLS - 1), b]
        pltpu.make_async_copy(several, several, row_recv.at[b]).wait()
        keep, state = one, none
        keep_before, state_before = keep, state
        for j in range(COLS):
            keep, state = row_buf[j, b, 0:1, :] * keep, row_buf[j, b, 0:1, :] * state + row_buf[j, b, 1:2, :]
            keep_before, state_before = jnp.where(j < col, keep, keep_before), jnp.where(j < col, state, state_before)
        before[b] = keep_before, state_before
        col_buf[row, b, 0:1, :] = keep
        col_buf[row, b, 1:2, :] = state
        for k in range(rows - 1):
            copy = pltpu.make_async_remote_copy(
                col_buf.at[row, b], col_buf.at[row, b], col_send, col_recv.at[b],
                device_id=col_peers[k], device_id_type=MESH,
            )
            pl.when(row + k + 1 < rows)(copy.start)

    def enter(b):
        for k in range(1, rows):
            several = col_buf.at[pl.ds(0, k), b]
            pl.when(row == k)(pltpu.make_async_copy(several, several, col_recv.at[b]).wait)
        state = none
        for j in range(rows):
            state = jnp.where(j < row, col_buf[j, b, 0:1, :] * state + col_buf[j, b, 1:2, :], state)
        keep_before, state_before = before[b]
        return keep_before * state + state_before

    def gate_block(block):
        local[block] = jnp.dot(lower[...], drives[block].reshape(2 * BLOCK, width), preferred_element_type=F32)
        for here in chunks:
            opening = jnp.tanh((gate[block, here, :] * 0.5).astype(F32)) + 1.0
            logs[block, here, :] = jnp.exp2(logs[block, here, :]) * opening

    def gate_batch(b):
        for block in range(b * halves, (b + 1) * halves):
            gates[block].wait()
        for block in range(b * halves, (b + 1) * halves):
            gate_block(block)

    def finish(b):
        start = enter(b)
        powers = jnp.zeros((halves, BLOCK), F32)
        for part in range(halves):
            block, where = b * halves + part, part * BLOCK
            squares = []
            for here in chunks:
                gated = logs[block, here, :] * (local[block, here, :] + start)
                gated_ref[b, where + here.start : where + here.stop, :] = gated
                square = gated * gated
                square = sum(square[:, k : k + LANES] for k in range(0, width, LANES))
                squares.append(jnp.concatenate(parts(square), axis=1))
            pick = jnp.where(iota((halves, 2 * LANES), 0) == part, 1.0, 0.0).astype(BF16)
            powers = powers + lax.dot_general(
                pick, jnp.concatenate(squares, axis=0), NT, preferred_element_type=F32
            )
            if part + 1 < halves:
                start = ends[block : block + 1, :] * (local[block, BLOCK - 1 :, :] + start)
        power_buf[chan, b] = powers
        for peer in chan_peers:
            pltpu.make_async_remote_copy(
                power_buf.at[chan, b], power_buf.at[chan, b], power_send, power_recv,
                device_id=peer, device_id_type=MESH,
            ).start()

    decays[0].wait()
    prepare(0)
    for block in range(blocks):
        if block + 1 < blocks:
            decays[block + 1].wait()
        driving[block].wait()
        if block == blocks // 2:
            for copy in gates[:blocks // 2]:
                copy.start()
        grow(block)
        if block + 1 < blocks:
            prepare(block + 1)
        if block % halves == halves - 1 and block + 1 < blocks:
            send_row(block // halves)
            if block + 1 + halves == blocks:
                pl.semaphore_wait(barrier, len(peers))
                for b in range(batch - 1):
                    start_row(b)
    send_row(batch - 1)
    start_row(batch - 1)
    for copy in gates[blocks // 2 :]:
        copy.start()

    for b in range(batch):
        gate_batch(b)
    for b in range(batch):
        send_col(b)
    for b in range(batch):
        finish(b)

    several = power_buf.at[pl.ds(0, chans - 1)]
    pltpu.make_async_copy(several, several, power_recv).wait()
    for b in range(batch):
        power = sum(power_buf[j, b] for j in range(chans)) * (half * half / (width * chans))
        scale_ref[b * halves : (b + 1) * halves, :] = half * lax.rsqrt(power + 1e-06)

    several = row_buf.at[pl.ds(0, COLS - 1)]
    pltpu.make_async_copy(several, several, row_send).wait()
    for k in range(1, rows):
        several = col_buf.at[pl.ds(0, k)]
        pl.when(row + k + 1 == rows)(pltpu.make_async_copy(several, several, col_send).wait)
    several = power_buf.at[pl.ds(0, chans - 1)]
    pltpu.make_async_copy(several, several, power_send).wait()


def scale_kernel(gated_ref, scale_ref, gain_ref, out_hbm, result, factors, sem):
    batch, length, width = result.shape
    blocks = scale_ref.shape[0]
    halves = blocks // batch
    wide = (2 * blocks, blocks * LANES)
    pick = jnp.where(lax.rem(iota(wide, 0), blocks) == iota(wide, 1) // LANES, 1.0, 0.0).astype(BF16)
    factors[...] = lax.dot_general(
        jnp.concatenate(parts(scale_ref[...]), axis=0), pick, TN, preferred_element_type=F32
    )
    gain = gain_ref[...].reshape(1, width)
    for block in range(blocks):
        b, where = block // halves, block % halves * BLOCK
        for k in range(0, BLOCK, CHUNK):
            here = slice(where + k, where + k + CHUNK)
            factor = factors[k : k + CHUNK, block * LANES : (block + 1) * LANES]
            factor = jnp.concatenate([factor] * (width // LANES), axis=1)
            result[b, here, :] = (gated_ref[b, here, :] * factor * gain).astype(result.dtype)
        there = (b, pl.ds(where, BLOCK))
        pltpu.make_async_copy(result.at[there], out_hbm.at[there], sem).start()
    pltpu.make_async_copy(result, out_hbm, sem).wait()


def solution(mesh):
    times, chans = mesh.shape["time"], mesh.shape["chan"]

    def body(decay_rate, drive_in, gate_in, norm_gain):
        batch, length, width = decay_rate.shape
        blocks = batch * length // BLOCK
        rows = times // COLS
        dma = pltpu.SemaphoreType.DMA
        vmem = pl.BlockSpec(memory_space=pltpu.VMEM)
        gated, scale = pl.pallas_call(
            functools.partial(state_kernel, times, chans),
            out_shape=(pltpu.VMEM((batch, length, width), F32), pltpu.VMEM((blocks, BLOCK), F32)),
            in_specs=[pl.BlockSpec(memory_space=pltpu.HBM)] * 3,
            out_specs=(vmem, vmem),
            scratch_shapes=[
                pltpu.VMEM((blocks, BLOCK, width), F32),
                pltpu.VMEM((blocks, 2, BLOCK, width), BF16),
                pltpu.VMEM((blocks, BLOCK, width), BF16),
                pltpu.VMEM((blocks, BLOCK, width), F32),
                pltpu.VMEM((blocks, BLOCK, width), F32),
                pltpu.VMEM((2, BLOCK, width), BF16),
                pltpu.VMEM((BLOCK, BLOCK), BF16),
                pltpu.VMEM((BLOCK, 2 * BLOCK), BF16),
                pltpu.VMEM((2 * blocks, width), F32),
                pltpu.VMEM((COLS, batch, 2, width), F32),
                pltpu.VMEM((rows, batch, 2, width), F32),
                pltpu.VMEM((chans, batch, length // BLOCK, BLOCK), F32),
                dma((blocks,)), dma((blocks,)),
                dma, dma((batch,)),
                dma, dma((batch,)),
                dma, dma,
            ],
            compiler_params=pltpu.CompilerParams(
                collective_id=0, has_side_effects=True, vmem_limit_bytes=57 * 2**20
            ),
        )(decay_rate, drive_in, gate_in)
        return pl.pallas_call(
            scale_kernel,
            out_shape=jax.ShapeDtypeStruct((batch, length, width), BF16),
            in_specs=[vmem, vmem, vmem],
            out_specs=pl.BlockSpec(memory_space=pltpu.HBM),
            scratch_shapes=[
                pltpu.VMEM((batch, length, width), BF16),
                pltpu.VMEM((BLOCK, blocks * LANES), F32),
                dma,
            ],
            compiler_params=pltpu.CompilerParams(vmem_limit_bytes=16 * 2**20),
        )(gated, scale, norm_gain)

    in_specs = (P(None, "time", "chan"), P(None, "time", "chan"), P(None, "time", "chan"), P("chan"))
    return jax.shard_map(body, mesh=mesh, in_specs=in_specs, out_specs=P(None, "time", "chan"), check_vma=False)
```

```python
import functools
import math

import jax
import jax.numpy as jnp
from jax import lax
from jax.experimental import pallas as pl
from jax.experimental.pallas import tpu as pltpu
from jax.sharding import PartitionSpec as P

MESH = pl.DeviceIdType.MESH
BLOCK = 256
LANES = 128
CHUNK = 16
COLS = 8
F32 = jnp.float32
BF16 = jnp.bfloat16
NT = (((1,), (1,)), ((), ()))
TN = (((0,), (0,)), ((), ()))


def iota(shape, dim):
    return lax.broadcasted_iota(jnp.int32, shape, dim)


def triangle(width, value):
    row, column = iota((BLOCK, width), 0), iota((BLOCK, width), 1)
    return jnp.where(lax.rem(column, BLOCK) <= row, value, 0.0).astype(BF16)


def parts(x):
    high = x.astype(BF16)
    return high, (x - high.astype(F32)).astype(BF16)


def state_kernel(
    times, chans, decay_hbm, drive_hbm, gate_hbm, gated_ref, scale_ref,
    decay, drives, gate, logs, local, rounded, fall, lower, ends, row_buf, col_buf, power_buf,
    decay_sem, drive_sem, row_send, row_recv, col_send, col_recv, power_send, power_recv,
):
    batch, length, width = decay_hbm.shape
    halves = length // BLOCK
    blocks = batch * halves
    rows = times // COLS
    total_length = length * times
    log2_scale = math.log2(math.e) / total_length
    half = 0.5 * total_length**-0.5
    time, chan = lax.axis_index("time"), lax.axis_index("chan")
    row, col = time // COLS, lax.rem(time, COLS)

    def at(ref, block):
        return ref.at[block // halves, pl.ds(block % halves * BLOCK, BLOCK), :]

    decays = [pltpu.make_async_copy(at(decay_hbm, k), decay.at[k], decay_sem.at[k]) for k in range(blocks)]
    driving = [pltpu.make_async_copy(at(drive_hbm, k), drives.at[k, 0], drive_sem.at[k]) for k in range(blocks)]
    gates = [pltpu.make_async_copy(at(gate_hbm, k), gate.at[k], decay_sem.at[k]) for k in range(blocks)]
    decays[0].start()
    for k in range(blocks):
        if k + 1 < blocks:
            decays[k + 1].start()
        driving[k].start()

    row_peers = [(row * COLS + lax.rem(col + k, COLS), chan) for k in range(1, COLS)]
    col_peers = [(lax.rem(row + k, rows) * COLS + col, chan) for k in range(1, rows)]
    chan_peers = [(time, lax.rem(chan + k, chans)) for k in range(1, chans)]
    peers = row_peers + col_peers + chan_peers
    barrier = pltpu.get_barrier_semaphore()
    for peer in peers:
        pl.semaphore_signal(barrier, inc=1, device_id=peer, device_id_type=MESH)

    fall[...] = triangle(BLOCK, log2_scale)
    lower[...] = triangle(2 * BLOCK, 1.0)
    chunks = [slice(k, k + CHUNK) for k in range(0, BLOCK, CHUNK)]
    none = jnp.zeros((1, width), F32)
    one = jnp.ones((1, width), F32)

    def prepare(block):
        total = jnp.zeros((8, width), F32)
        for here in chunks:
            rate = decay[block, here, :]
            total = total + (rate[:8] + rate[8:])
            rounded[block % 2, here, :] = rate.astype(BF16)
        ends[block : block + 1, :] = jnp.exp2(total.sum(0, keepdims=True) * -log2_scale)

    def mixed(block):
        total = jnp.zeros((8, width), F32)
        pieces = [(0, 256, chunks[:3]), (256, 512, chunks[3:6]), (512, width, chunks[6:])]
        for left, right, some in pieces:
            if block + 1 < blocks:
                logs[block + 1, :, left:right] = jnp.dot(
                    fall[...], rounded[(block + 1) % 2, :, left:right], preferred_element_type=F32
                )
            for here in some:
                drive, growth = drives[block, 0, here, :], jnp.exp2(logs[block, here, :])
                grown = drive.astype(F32) * growth
                total = total + (grown[:8] + grown[8:])
        ends[blocks + block : blocks + block + 1, :] = ends[block : block + 1, :] * total.sum(0, keepdims=True)

    def send_row(b):
        keep, state = one, none
        for k in range(b * halves, (b + 1) * halves):
            shrink = ends[k : k + 1, :]
            keep, state = shrink * keep, shrink * state + ends[blocks + k : blocks + k + 1, :]
        row_buf[col, b, 0:1, :] = keep
        row_buf[col, b, 1:2, :] = state

    def start_row(b):
        for peer in row_peers:
            pltpu.make_async_remote_copy(
                row_buf.at[col, b], row_buf.at[col, b], row_send, row_recv.at[b],
                device_id=peer, device_id_type=MESH,
            ).start()

    before = {}

    def send_col(b):
        several = row_buf.at[pl.ds(0, COLS - 1), b]
        pltpu.make_async_copy(several, several, row_recv.at[b]).wait()
        keep, state = one, none
        keep_before, state_before = keep, state
        for j in range(COLS):
            keep, state = row_buf[j, b, 0:1, :] * keep, row_buf[j, b, 0:1, :] * state + row_buf[j, b, 1:2, :]
            keep_before, state_before = jnp.where(j < col, keep, keep_before), jnp.where(j < col, state, state_before)
        before[b] = keep_before, state_before
        col_buf[row, b, 0:1, :] = keep
        col_buf[row, b, 1:2, :] = state
        for k in range(rows - 1):
            copy = pltpu.make_async_remote_copy(
                col_buf.at[row, b], col_buf.at[row, b], col_send, col_recv.at[b],
                device_id=col_peers[k], device_id_type=MESH,
            )
            pl.when(row + k + 1 < rows)(copy.start)

    def wait_col(b):
        for k in range(1, rows):
            several = col_buf.at[pl.ds(0, k), b]
            pl.when(row == k)(pltpu.make_async_copy(several, several, col_recv.at[b]).wait)

    def enter(b):
        state = none
        for j in range(rows):
            state = jnp.where(j < row, col_buf[j, b, 0:1, :] * state + col_buf[j, b, 1:2, :], state)
        keep_before, state_before = before[b]
        return keep_before * state + state_before

    def gate_block(block):
        local[block] = jnp.dot(lower[...], drives[block].reshape(2 * BLOCK, width), preferred_element_type=F32)
        for here in chunks:
            opening = jnp.tanh((gate[block, here, :] * 0.5).astype(F32)) + 1.0
            logs[block, here, :] = jnp.exp2(-logs[block, here, :]) * opening

    def spread(b):
        for block in range(b * halves, (b + 1) * halves):
            for here in chunks:
                growth = jnp.exp2(logs[block, here, :]) - 1.0
                drives[block, 1, here, :] = growth.astype(BF16) * drives[block, 0, here, :]

    def gate_batch(b):
        for block in range(b * halves, (b + 1) * halves):
            gates[block].wait()
        for block in range(b * halves, (b + 1) * halves):
            gate_block(block)
        if b + 1 < batch:
            spread(b + 1)

    def finish(b):
        start = enter(b)
        powers = jnp.zeros((halves, BLOCK), F32)
        for part in range(halves):
            block, where = b * halves + part, part * BLOCK
            squares = []
            for here in chunks:
                gated = logs[block, here, :] * (local[block, here, :] + start)
                gated_ref[b, where + here.start : where + here.stop, :] = gated
                square = gated * gated
                square = sum(square[:, k : k + LANES] for k in range(0, width, LANES))
                squares.append(jnp.concatenate(parts(square), axis=1))
            pick = jnp.where(iota((halves, 2 * LANES), 0) == part, 1.0, 0.0).astype(BF16)
            powers = powers + lax.dot_general(
                pick, jnp.concatenate(squares, axis=0), NT, preferred_element_type=F32
            )
            if part + 1 < halves:
                start = ends[block : block + 1, :] * (local[block, BLOCK - 1 :, :] + start)
        power_buf[chan, b] = powers

    def send_power(b):
        for peer in chan_peers:
            pltpu.make_async_remote_copy(
                power_buf.at[chan, b], power_buf.at[chan, b], power_send, power_recv,
                device_id=peer, device_id_type=MESH,
            ).start()

    decays[0].wait()
    prepare(0)
    decays[1].wait()
    logs[0] = jnp.dot(fall[...], rounded[0], preferred_element_type=F32)
    prepare(1)
    for block in range(blocks):
        if block + 2 < blocks:
            decays[block + 2].wait()
        driving[block].wait()
        if block == blocks // 2:
            for copy in gates[:blocks // 2]:
                copy.start()
        mixed(block)
        if block + 2 < blocks:
            prepare(block + 2)
        if block % halves == halves - 1 and block + 1 < blocks:
            b = block // halves
            send_row(b)
            if b == 1:
                pl.semaphore_wait(barrier, len(peers))
                start_row(0)
            if b >= 1:
                start_row(b)
    send_row(batch - 1)
    start_row(batch - 1)
    for copy in gates[blocks // 2 :]:
        copy.start()

    spread(0)
    for b in range(batch):
        gate_batch(b)
    for b in range(batch):
        send_col(b)
    for group in (range(2), range(2, batch)):
        for b in group:
            wait_col(b)
        for b in group:
            finish(b)
        for b in group:
            send_power(b)

    several = row_buf.at[pl.ds(0, COLS - 1)]
    pltpu.make_async_copy(several, several, row_send).wait()
    for k in range(1, rows):
        several = col_buf.at[pl.ds(0, k)]
        pl.when(row + k + 1 == rows)(pltpu.make_async_copy(several, several, col_send).wait)
    several = power_buf.at[pl.ds(0, chans - 1)]
    pltpu.make_async_copy(several, several, power_send).wait()
    pltpu.make_async_copy(several, several, power_recv).wait()
    for b in range(batch):
        power = sum(power_buf[j, b] for j in range(chans)) * (half * half / (width * chans))
        scale_ref[b * halves : (b + 1) * halves, :] = half * lax.rsqrt(power + 1e-06)


def scale_kernel(gated_ref, scale_ref, gain_ref, out_hbm, result, factors, sem):
    batch, length, width = result.shape
    blocks = scale_ref.shape[0]
    halves = blocks // batch
    wide = (2 * blocks, blocks * LANES)
    pick = jnp.where(lax.rem(iota(wide, 0), blocks) == iota(wide, 1) // LANES, 1.0, 0.0).astype(BF16)
    factors[...] = lax.dot_general(
        jnp.concatenate(parts(scale_ref[...]), axis=0), pick, TN, preferred_element_type=F32
    )
    gain = jnp.broadcast_to(gain_ref[...].reshape(1, width), (8, width))

    def write(block, carry):
        b, where = block // halves, lax.rem(block, halves) * BLOCK
        lane = pl.ds(pl.multiple_of(block * LANES, LANES), LANES)
        for k in range(0, BLOCK, CHUNK):
            here = pl.ds(pl.multiple_of(where + k, CHUNK), CHUNK)
            factor = jnp.concatenate([factors[k : k + CHUNK, lane]] * (width // LANES), axis=1)
            factor = factor * jnp.concatenate([gain] * (CHUNK // 8), axis=0)
            result[b, here, :] = (gated_ref[b, here, :] * factor).astype(result.dtype)
        there = (b, pl.ds(pl.multiple_of(where, BLOCK), BLOCK))
        pltpu.make_async_copy(result.at[there], out_hbm.at[there], sem).start()
        return carry

    lax.fori_loop(0, blocks, write, 0)
    pltpu.make_async_copy(result, out_hbm, sem).wait()


def solution(mesh):
    times, chans = mesh.shape["time"], mesh.shape["chan"]

    def body(decay_rate, drive_in, gate_in, norm_gain):
        batch, length, width = decay_rate.shape
        blocks = batch * length // BLOCK
        rows = times // COLS
        dma = pltpu.SemaphoreType.DMA
        vmem = pl.BlockSpec(memory_space=pltpu.VMEM)
        gated, scale = pl.pallas_call(
            functools.partial(state_kernel, times, chans),
            out_shape=(pltpu.VMEM((batch, length, width), F32), pltpu.VMEM((blocks, BLOCK), F32)),
            in_specs=[pl.BlockSpec(memory_space=pltpu.HBM)] * 3,
            out_specs=(vmem, vmem),
            scratch_shapes=[
                pltpu.VMEM((blocks, BLOCK, width), F32),
                pltpu.VMEM((blocks, 2, BLOCK, width), BF16),
                pltpu.VMEM((blocks, BLOCK, width), BF16),
                pltpu.VMEM((blocks, BLOCK, width), F32),
                pltpu.VMEM((blocks, BLOCK, width), F32),
                pltpu.VMEM((2, BLOCK, width), BF16),
                pltpu.VMEM((BLOCK, BLOCK), BF16),
                pltpu.VMEM((BLOCK, 2 * BLOCK), BF16),
                pltpu.VMEM((2 * blocks, width), F32),
                pltpu.VMEM((COLS, batch, 2, width), F32),
                pltpu.VMEM((rows, batch, 2, width), F32),
                pltpu.VMEM((chans, batch, length // BLOCK, BLOCK), F32),
                dma((blocks,)), dma((blocks,)),
                dma, dma((batch,)),
                dma, dma((batch,)),
                dma, dma,
            ],
            compiler_params=pltpu.CompilerParams(
                collective_id=0, has_side_effects=True, vmem_limit_bytes=57 * 2**20
            ),
        )(decay_rate, drive_in, gate_in)
        return pl.pallas_call(
            scale_kernel,
            out_shape=jax.ShapeDtypeStruct((batch, length, width), BF16),
            in_specs=[vmem, vmem, vmem],
            out_specs=pl.BlockSpec(memory_space=pltpu.HBM),
            scratch_shapes=[
                pltpu.VMEM((batch, length, width), BF16),
                pltpu.VMEM((BLOCK, blocks * LANES), F32),
                dma,
            ],
            compiler_params=pltpu.CompilerParams(vmem_limit_bytes=16 * 2**20),
        )(gated, scale, norm_gain)

    in_specs = (P(None, "time", "chan"), P(None, "time", "chan"), P(None, "time", "chan"), P("chan"))
    return jax.shard_map(body, mesh=mesh, in_specs=in_specs, out_specs=P(None, "time", "chan"), check_vma=False)
```

```python
import functools
import math

import jax
import jax.numpy as jnp
from jax import lax
from jax.experimental import pallas as pl
from jax.experimental.pallas import tpu as pltpu
from jax.sharding import PartitionSpec as P

MESH = pl.DeviceIdType.MESH
BLOCK = 256
LANES = 128
CHUNK = 16
COLS = 8
CORES = 2
F32 = jnp.float32
BF16 = jnp.bfloat16
NT = (((1,), (1,)), ((), ()))
TN = (((0,), (0,)), ((), ()))


def iota(shape, dim):
    return lax.broadcasted_iota(jnp.int32, shape, dim)


def triangle(width, value):
    row, column = iota((BLOCK, width), 0), iota((BLOCK, width), 1)
    return jnp.where(lax.rem(column, BLOCK) <= row, value, 0.0).astype(BF16)


def parts(x):
    high = x.astype(BF16)
    return high, (x - high.astype(F32)).astype(BF16)


def state_kernel(
    times, chans, decay_hbm, drive_hbm, gate_hbm, gain_hbm, gated_ref, scale_ref,
    decay, drives, gate, gain, logs, local, rounded, fall, lower, ends, row_buf, col_buf, power_buf,
    load_sem, row_send, row_recv, col_send, col_recv, power_send, power_recv,
):
    batch, length, width = decay_hbm.shape
    halves = length // BLOCK
    blocks = batch * halves
    rows = times // COLS
    total_length = length * times
    log2_scale = math.log2(math.e) / total_length
    half = 0.5 * total_length**-0.5
    time, chan = lax.axis_index("time"), lax.axis_index("chan")
    row, col = time // COLS, lax.rem(time, COLS)

    def at(ref, block):
        return ref.at[block // halves, pl.ds(block % halves * BLOCK, BLOCK), :]

    def load(source, target, slot):
        return pltpu.make_async_copy(source, target, load_sem.at[slot])

    def wait_pair(slot, halves_of_pair):
        several = drives.at[pl.ds(0, halves_of_pair), 0]
        pltpu.make_async_copy(several, several, load_sem.at[slot]).wait()

    decays = [load(at(decay_hbm, k), decay.at[k], k) for k in range(blocks)]
    driving = [load(at(drive_hbm, k), drives.at[k, 0], k + 2) for k in range(blocks)]
    gates = [load(at(gate_hbm, k), gate.at[k], k // halves) for k in range(blocks)]
    gains = load(gain_hbm, gain, blocks + 2)
    decays[0].start()
    decays[1].start()
    for k in range(blocks):
        driving[k].start()
        if k + 2 < blocks:
            decays[k + 2].start()

    chips = COLS // CORES
    chip, core = col // CORES, lax.rem(col, CORES)
    leads = core == CORES - 1
    row_peers = [
        (row * COLS + lax.rem(chip + k, chips) * CORES + c, chan) for c in reversed(range(CORES)) for k in range(1, chips)
    ]
    row_peers += [(row * COLS + chip * CORES + lax.rem(core + k, CORES), chan) for k in range(1, CORES)]
    col_peers = [
        (lax.rem(row + k, rows) * COLS + chip * CORES + c, chan) for k in range(1, rows) for c in range(CORES)
    ]
    chan_peers = [(time, lax.rem(chan + k, chans)) for k in range(1, chans)]
    peers = row_peers + col_peers + chan_peers
    barrier = pltpu.get_barrier_semaphore()
    for peer in peers:
        pl.semaphore_signal(barrier, inc=1, device_id=peer, device_id_type=MESH)

    fall[...] = triangle(BLOCK, log2_scale)
    lower[...] = triangle(2 * BLOCK, 1.0)
    chunks = [slice(k, k + CHUNK) for k in range(0, BLOCK, CHUNK)]
    none = jnp.zeros((1, width), F32)
    one = jnp.ones((1, width), F32)

    def prepare(block):
        total = jnp.zeros((8, width), F32)
        for here in chunks:
            rate = decay[block, here, :]
            total = total + (rate[:8] + rate[8:])
            rounded[block % 2, here, :] = rate.astype(BF16)
        ends[block : block + 1, :] = jnp.exp2(total.sum(0, keepdims=True) * -log2_scale)

    def mixed(block):
        total = jnp.zeros((8, width), F32)
        pieces = [(0, 256, chunks[:3]), (256, 512, chunks[3:6]), (512, width, chunks[6:])]
        for left, right, some in pieces:
            if block + 1 < blocks:
                logs[block + 1, :, left:right] = jnp.dot(
                    fall[...], rounded[(block + 1) % 2, :, left:right], preferred_element_type=F32
                )
            for here in some:
                drive, growth = drives[block, 0, here, :], jnp.exp2(logs[block, here, :])
                grown = drive.astype(F32) * growth
                total = total + (grown[:8] + grown[8:])
        ends[blocks + block : blocks + block + 1, :] = ends[block : block + 1, :] * total.sum(0, keepdims=True)

    def send_row(b):
        keep, state = one, none
        for k in range(b * halves, (b + 1) * halves):
            shrink = ends[k : k + 1, :]
            keep, state = shrink * keep, shrink * state + ends[blocks + k : blocks + k + 1, :]
        row_buf[col, b, 0:1, :] = keep
        row_buf[col, b, 1:2, :] = state

    def start_row(b):
        for peer in row_peers:
            pltpu.make_async_remote_copy(
                row_buf.at[col, b], row_buf.at[col, b], row_send, row_recv.at[b],
                device_id=peer, device_id_type=MESH,
            ).start()

    before = {}

    def send_col(b):
        several = row_buf.at[pl.ds(0, COLS - 1), b]
        pltpu.make_async_copy(several, several, row_recv.at[b]).wait()
        keep, state = one, none
        keep_before, state_before = keep, state
        for j in range(COLS):
            keep, state = row_buf[j, b, 0:1, :] * keep, row_buf[j, b, 0:1, :] * state + row_buf[j, b, 1:2, :]
            keep_before, state_before = jnp.where(j < col, keep, keep_before), jnp.where(j < col, state, state_before)
        before[b] = keep_before, state_before
        col_buf[row, b, 0:1, :] = keep
        col_buf[row, b, 1:2, :] = state
        for i, peer in enumerate(col_peers):
            copy = pltpu.make_async_remote_copy(
                col_buf.at[row, b], col_buf.at[row, b], col_send.at[i % CORES], col_recv.at[b],
                device_id=peer, device_id_type=MESH,
            )
            pl.when(jnp.logical_and(leads, row + i // CORES + 1 < rows))(copy.start)

    def wait_col(b):
        for k in range(1, rows):
            several = col_buf.at[pl.ds(0, k), b]
            pl.when(row == k)(pltpu.make_async_copy(several, several, col_recv.at[b]).wait)

    def enter(b):
        state = none
        for j in range(rows):
            state = jnp.where(j < row, col_buf[j, b, 0:1, :] * state + col_buf[j, b, 1:2, :], state)
        keep_before, state_before = before[b]
        return keep_before * state + state_before

    def gate_block(block):
        local[block] = jnp.dot(lower[...], drives[block].reshape(2 * BLOCK, width), preferred_element_type=F32)
        for here in chunks:
            opening = jnp.tanh((gate[block, here, :] * 0.5).astype(F32)) + 1.0
            logs[block, here, :] = jnp.exp2(-logs[block, here, :]) * opening

    def spread(b):
        for block in range(b * halves, (b + 1) * halves):
            for here in chunks:
                growth = jnp.exp2(logs[block, here, :]) - 1.0
                drives[block, 1, here, :] = growth.astype(BF16) * drives[block, 0, here, :]

    def gate_batch(b):
        wait_pair(b, halves)
        for block in range(b * halves, (b + 1) * halves):
            gate_block(block)
        if b + 1 < batch:
            spread(b + 1)

    def finish(b):
        start = enter(b)
        powers = jnp.zeros((halves, BLOCK), F32)
        for part in range(halves):
            block, where = b * halves + part, part * BLOCK
            squares = []
            for here in chunks:
                gated = logs[block, here, :] * (local[block, here, :] + start)
                gated_ref[b, where + here.start : where + here.stop, :] = gated
                square = gated * gated
                square = sum(square[:, k : k + LANES] for k in range(0, width, LANES))
                squares.append(jnp.concatenate(parts(square), axis=1))
            pick = jnp.where(iota((halves, 2 * LANES), 0) == part, 1.0, 0.0).astype(BF16)
            powers = powers + lax.dot_general(
                pick, jnp.concatenate(squares, axis=0), NT, preferred_element_type=F32
            )
            if part + 1 < halves:
                start = ends[block : block + 1, :] * (local[block, BLOCK - 1 :, :] + start)
        power_buf[chan, b] = powers

    def send_power(b):
        for peer in chan_peers:
            pltpu.make_async_remote_copy(
                power_buf.at[chan, b], power_buf.at[chan, b], power_send, power_recv,
                device_id=peer, device_id_type=MESH,
            ).start()

    decays[0].wait()
    prepare(0)
    logs[0] = jnp.dot(fall[...], rounded[0], preferred_element_type=F32)
    decays[1].wait()
    prepare(1)
    for block in range(blocks):
        wait_pair(block + 2, 3 if block + 2 < blocks else 1)
        if block == blocks // 2:
            for copy in gates[: blocks // 2]:
                copy.start()
        mixed(block)
        if block + 2 < blocks:
            prepare(block + 2)
        if block % halves == halves - 1 and block + 1 < blocks:
            b = block // halves
            send_row(b)
            if b == 1:
                pl.semaphore_wait(barrier, len(peers))
                start_row(0)
            if b >= 1:
                start_row(b)
    send_row(batch - 1)
    start_row(batch - 1)
    for copy in gates[blocks // 2 :]:
        copy.start()
    gains.start()

    spread(0)
    for b in range(batch):
        gate_batch(b)
    for b in range(batch):
        send_col(b)
    for group in (range(2), *([b] for b in range(2, batch))):
        for b in group:
            wait_col(b)
        for b in group:
            finish(b)
        for b in group:
            send_power(b)

    gains.wait()
    by_gain = jnp.broadcast_to(gain[...].reshape(1, width), (CHUNK, width))

    def weigh(i, carry):
        here = pl.ds(pl.multiple_of(i * CHUNK, CHUNK), CHUNK)
        for b in range(batch):
            gated_ref[b, here, :] = gated_ref[b, here, :] * by_gain
        return carry

    lax.fori_loop(0, length // CHUNK, weigh, 0)

    several = row_buf.at[pl.ds(0, COLS - 1)]
    pltpu.make_async_copy(several, several, row_send).wait()
    for k in range(1, rows):
        several = col_buf.at[pl.ds(0, k)]
        for c in range(CORES):
            copy = pltpu.make_async_copy(several, several, col_send.at[c])
            pl.when(jnp.logical_and(leads, row + k + 1 == rows))(copy.wait)
    several = power_buf.at[pl.ds(0, chans - 1)]
    pltpu.make_async_copy(several, several, power_send).wait()
    pltpu.make_async_copy(several, several, power_recv).wait()
    for b in range(batch):
        power = sum(power_buf[j, b] for j in range(chans)) * (half * half / (width * chans))
        scale_ref[b * halves : (b + 1) * halves, :] = half * lax.rsqrt(power + 1e-06)


def scale_kernel(gated_ref, scale_ref, out_hbm, result, factors, sem):
    batch, length, width = result.shape
    blocks = scale_ref.shape[0]
    halves = blocks // batch
    wide = (2 * blocks, blocks * LANES)
    pick = jnp.where(lax.rem(iota(wide, 0), blocks) == iota(wide, 1) // LANES, 1.0, 0.0).astype(BF16)
    factors[...] = lax.dot_general(
        jnp.concatenate(parts(scale_ref[...]), axis=0), pick, TN, preferred_element_type=F32
    )

    def write(block, carry):
        b, where = block // halves, lax.rem(block, halves) * BLOCK
        lane = pl.ds(pl.multiple_of(block * LANES, LANES), LANES)
        for k in range(0, BLOCK, CHUNK):
            here = pl.ds(pl.multiple_of(where + k, CHUNK), CHUNK)
            factor = jnp.concatenate([factors[k : k + CHUNK, lane]] * (width // LANES), axis=1)
            result[b, here, :] = (gated_ref[b, here, :] * factor).astype(result.dtype)
        there = (b, pl.ds(pl.multiple_of(where, BLOCK), BLOCK))
        pltpu.make_async_copy(result.at[there], out_hbm.at[there], sem).start()
        return carry

    lax.fori_loop(0, blocks, write, 0)
    pltpu.make_async_copy(result, out_hbm, sem).wait()


def solution(mesh):
    times, chans = mesh.shape["time"], mesh.shape["chan"]

    def body(decay_rate, drive_in, gate_in, norm_gain):
        batch, length, width = decay_rate.shape
        blocks = batch * length // BLOCK
        rows = times // COLS
        dma = pltpu.SemaphoreType.DMA
        vmem = pl.BlockSpec(memory_space=pltpu.VMEM)
        gated, scale = pl.pallas_call(
            functools.partial(state_kernel, times, chans),
            out_shape=(pltpu.VMEM((batch, length, width), F32), pltpu.VMEM((blocks, BLOCK), F32)),
            in_specs=[pl.BlockSpec(memory_space=pltpu.HBM)] * 4,
            out_specs=(vmem, vmem),
            scratch_shapes=[
                pltpu.VMEM((blocks, BLOCK, width), F32),
                pltpu.VMEM((blocks, 2, BLOCK, width), BF16),
                pltpu.VMEM((blocks, BLOCK, width), BF16),
                pltpu.VMEM((width,), F32),
                pltpu.VMEM((blocks, BLOCK, width), F32),
                pltpu.VMEM((blocks, BLOCK, width), F32),
                pltpu.VMEM((2, BLOCK, width), BF16),
                pltpu.VMEM((BLOCK, BLOCK), BF16),
                pltpu.VMEM((BLOCK, 2 * BLOCK), BF16),
                pltpu.VMEM((2 * blocks, width), F32),
                pltpu.VMEM((COLS, batch, 2, width), F32),
                pltpu.VMEM((rows, batch, 2, width), F32),
                pltpu.VMEM((chans, batch, length // BLOCK, BLOCK), F32),
                dma((blocks + 3,)),
                dma, dma((batch,)),
                dma((CORES,)), dma((batch,)),
                dma, dma,
            ],
            compiler_params=pltpu.CompilerParams(
                collective_id=0, has_side_effects=True, vmem_limit_bytes=57 * 2**20
            ),
        )(decay_rate, drive_in, gate_in, norm_gain)
        return pl.pallas_call(
            scale_kernel,
            out_shape=jax.ShapeDtypeStruct((batch, length, width), BF16),
            in_specs=[vmem, vmem],
            out_specs=pl.BlockSpec(memory_space=pltpu.HBM),
            scratch_shapes=[
                pltpu.VMEM((batch, length, width), BF16),
                pltpu.VMEM((BLOCK, blocks * LANES), F32),
                dma,
            ],
            compiler_params=pltpu.CompilerParams(vmem_limit_bytes=16 * 2**20),
        )(gated, scale)

    in_specs = (P(None, "time", "chan"), P(None, "time", "chan"), P(None, "time", "chan"), P("chan"))
    return jax.shard_map(body, mesh=mesh, in_specs=in_specs, out_specs=P(None, "time", "chan"), check_vma=False)
```

```python
import functools
import math

import jax
import jax.numpy as jnp
from jax import lax
from jax.experimental import pallas as pl
from jax.experimental.pallas import tpu as pltpu
from jax.sharding import PartitionSpec as P

MESH = pl.DeviceIdType.MESH
BLOCK = 256
LANES = 128
CHUNK = 16
COLS = 8
CORES = 2
F32 = jnp.float32
BF16 = jnp.bfloat16
NT = (((1,), (1,)), ((), ()))
TN = (((0,), (0,)), ((), ()))


def iota(shape, dim):
    return lax.broadcasted_iota(jnp.int32, shape, dim)


def triangle(width, value):
    row, column = iota((BLOCK, width), 0), iota((BLOCK, width), 1)
    return jnp.where(lax.rem(column, BLOCK) <= row, value, 0.0).astype(BF16)


def parts(x):
    high = x.astype(BF16)
    return high, (x - high.astype(F32)).astype(BF16)


def state_kernel(
    times, chans, decay_hbm, drive_hbm, gate_hbm, gain_hbm, gated_ref, scale_ref,
    decay, drives, gate, gain, logs, local, rounded, fall, lower, ends, starts, row_buf, col_buf, before, hand_buf, power_buf,
    load_sem, row_send, row_recv, hand_send, hand_recv, col_send, col_recv, power_send, power_recv,
):
    batch, length, width = decay_hbm.shape
    halves = length // BLOCK
    blocks = batch * halves
    rows = times // COLS
    total_length = length * times
    log2_scale = math.log2(math.e) / total_length
    half = 0.5 * total_length**-0.5
    time, chan = lax.axis_index("time"), lax.axis_index("chan")
    row, col = time // COLS, lax.rem(time, COLS)

    def at(ref, block):
        return ref.at[block // halves, pl.ds(block % halves * BLOCK, BLOCK), :]

    def load(source, target, slot):
        return pltpu.make_async_copy(source, target, load_sem.at[slot])

    def wait_pair(slot, halves_of_pair):
        several = drives.at[pl.ds(0, halves_of_pair), 0]
        pltpu.make_async_copy(several, several, load_sem.at[slot]).wait()

    decays = [load(at(decay_hbm, k), decay.at[k], k) for k in range(blocks)]
    driving = [load(at(drive_hbm, k), drives.at[k, 0], k + 2) for k in range(blocks)]
    gates = [load(at(gate_hbm, k), gate.at[k], k // halves) for k in range(blocks)]
    gains = load(gain_hbm, gain, blocks + 2)
    decays[0].start()
    decays[1].start()
    for k in range(blocks):
        driving[k].start()
        if k + 2 < blocks:
            decays[k + 2].start()

    chips = COLS // CORES
    chip, core = col // CORES, lax.rem(col, CORES)
    leads = core == CORES - 1
    lead_of = [(row * COLS + lax.rem(chip + k, chips) * CORES + CORES - 1, chan) for k in range(chips)]
    mates = [(row * COLS + lax.rem(chip + k, chips) * CORES + c, chan) for k in range(1, chips) for c in range(CORES)]
    mate = (row * COLS + chip * CORES + CORES - 1 - core, chan)
    col_peers = [
        (lax.rem(row + k, rows) * COLS + chip * CORES + c, chan) for k in range(1, rows) for c in range(CORES)
    ]
    chan_peers = [(time, lax.rem(chan + k, chans)) for k in range(1, chans)]
    peers = mates + [mate] + col_peers + chan_peers
    barrier = pltpu.get_barrier_semaphore()
    for peer in peers:
        pl.semaphore_signal(barrier, inc=1, device_id=peer, device_id_type=MESH)

    fall[...] = triangle(BLOCK, log2_scale)
    lower[...] = triangle(2 * BLOCK, 1.0)
    chunks = [slice(k, k + CHUNK) for k in range(0, BLOCK, CHUNK)]
    none = jnp.zeros((1, width), F32)
    one = jnp.ones((1, width), F32)

    def prepare(block):
        total = jnp.zeros((8, width), F32)
        for here in chunks:
            rate = decay[block, here, :]
            total = total + (rate[:8] + rate[8:])
            rounded[block % 2, here, :] = rate.astype(BF16)
        ends[block : block + 1, :] = jnp.exp2(total.sum(0, keepdims=True) * -log2_scale)

    def mixed(block):
        total = jnp.zeros((8, width), F32)
        pieces = [(0, 256, chunks[:3]), (256, 512, chunks[3:6]), (512, width, chunks[6:])]
        for left, right, some in pieces:
            if block + 1 < blocks:
                logs[block + 1, :, left:right] = jnp.dot(
                    fall[...], rounded[(block + 1) % 2, :, left:right], preferred_element_type=F32
                )
            for here in some:
                drive, growth = drives[block, 0, here, :], jnp.exp2(logs[block, here, :])
                grown = drive.astype(F32) * growth
                total = total + (grown[:8] + grown[8:])
        ends[blocks + block : blocks + block + 1, :] = ends[block : block + 1, :] * total.sum(0, keepdims=True)

    def send_row(b):
        keep, state = one, none
        for k in range(b * halves, (b + 1) * halves):
            shrink = ends[k : k + 1, :]
            keep, state = shrink * keep, shrink * state + ends[blocks + k : blocks + k + 1, :]
        row_buf[col, b, 0:1, :] = keep
        row_buf[col, b, 1:2, :] = state

    def start_row(b):
        for k in range(1, chips):
            row_copy(b, lead_of[k]).start()
        pl.when(core == 0)(row_copy(b, lead_of[0]).start)

    def row_copy(b, peer):
        return pltpu.make_async_remote_copy(
            row_buf.at[col, b], row_buf.at[col, b], row_send, row_recv.at[b], device_id=peer, device_id_type=MESH
        )

    def handed(b):
        return pltpu.make_async_remote_copy(
            hand_buf.at[b], before.at[b], hand_send, hand_recv.at[b], device_id=mate, device_id_type=MESH
        )

    def send_col(b):
        several = row_buf.at[pl.ds(0, COLS - 1), b]
        pltpu.make_async_copy(several, several, row_recv.at[b]).wait()
        keep, state = one, none
        keep_chip, state_chip, keep_before, state_before = keep, state, keep, state
        for j in range(COLS):
            keep, state = row_buf[j, b, 0:1, :] * keep, row_buf[j, b, 0:1, :] * state + row_buf[j, b, 1:2, :]
            inside, earlier = j < col, j < chip * CORES
            keep_before, state_before = jnp.where(inside, keep, keep_before), jnp.where(inside, state, state_before)
            keep_chip, state_chip = jnp.where(earlier, keep, keep_chip), jnp.where(earlier, state, state_chip)
        col_buf[row, b, 0:1, :] = keep
        col_buf[row, b, 1:2, :] = state
        for i, peer in enumerate(col_peers):
            copy = pltpu.make_async_remote_copy(
                col_buf.at[row, b], col_buf.at[row, b], col_send.at[i % CORES], col_recv.at[b],
                device_id=peer, device_id_type=MESH,
            )
            pl.when(row + i // CORES + 1 < rows)(copy.start)
        before[b, 0:1, :] = keep_before
        before[b, 1:2, :] = state_before
        hand_buf[b, 0:1, :] = keep_chip
        hand_buf[b, 1:2, :] = state_chip
        handed(b).start()

    def wait_col(b):
        pl.when(core == 0)(handed(b).wait_recv)
        for k in range(1, rows):
            several = col_buf.at[pl.ds(0, k), b]
            pl.when(row == k)(pltpu.make_async_copy(several, several, col_recv.at[b]).wait)

    def enter(b):
        state = none
        for j in range(rows):
            state = jnp.where(j < row, col_buf[j, b, 0:1, :] * state + col_buf[j, b, 1:2, :], state)
        return before[b, 0:1, :] * state + before[b, 1:2, :]

    def gate_block(block):
        local[block] = jnp.dot(lower[...], drives[block].reshape(2 * BLOCK, width), preferred_element_type=F32)
        for here in chunks:
            opening = jnp.tanh((gate[block, here, :] * 0.5).astype(F32)) + 1.0
            logs[block, here, :] = jnp.exp2(-logs[block, here, :]) * opening

    def spread(b):
        for block in range(b * halves, (b + 1) * halves):
            for here in chunks:
                growth = jnp.exp2(logs[block, here, :]) - 1.0
                drives[block, 1, here, :] = growth.astype(BF16) * drives[block, 0, here, :]

    def gate_batch(b):
        wait_pair(b, halves)
        for block in range(b * halves, (b + 1) * halves):
            gate_block(block)
        if b + 1 < batch:
            spread(b + 1)

    def finish(b):
        start = enter(b)
        powers = jnp.zeros((halves, BLOCK), F32)
        for part in range(halves):
            block = b * halves + part
            starts[block : block + 1, :] = start
            squares = []
            for here in chunks:
                gated = logs[block, here, :] * (local[block, here, :] + start)
                square = gated * gated
                square = sum(square[:, k : k + LANES] for k in range(0, width, LANES))
                squares.append(jnp.concatenate(parts(square), axis=1))
            pick = jnp.where(iota((halves, 2 * LANES), 0) == part, 1.0, 0.0).astype(BF16)
            powers = powers + lax.dot_general(
                pick, jnp.concatenate(squares, axis=0), NT, preferred_element_type=F32
            )
            if part + 1 < halves:
                start = ends[block : block + 1, :] * (local[block, BLOCK - 1 :, :] + start)
        power_buf[chan, b] = powers

    def send_power(b):
        for peer in chan_peers:
            pltpu.make_async_remote_copy(
                power_buf.at[chan, b], power_buf.at[chan, b], power_send, power_recv,
                device_id=peer, device_id_type=MESH,
            ).start()

    decays[0].wait()
    prepare(0)
    logs[0] = jnp.dot(fall[...], rounded[0], preferred_element_type=F32)
    decays[1].wait()
    prepare(1)
    for block in range(blocks):
        wait_pair(block + 2, 3 if block + 2 < blocks else 1)
        if block == blocks // 2:
            for copy in gates[: blocks // 2]:
                copy.start()
        mixed(block)
        if block + 2 < blocks:
            prepare(block + 2)
        if block % halves == halves - 1 and block + 1 < blocks:
            b = block // halves
            send_row(b)
            if b == 1:
                pl.semaphore_wait(barrier, len(peers))
                start_row(0)
            if b >= 1:
                start_row(b)
    send_row(batch - 1)
    start_row(batch - 1)
    for copy in gates[blocks // 2 :]:
        copy.start()
    gains.start()

    spread(0)
    for b in range(batch - 1):
        gate_batch(b)
    for b in range(batch):
        pl.when(leads)(functools.partial(send_col, b))
    gate_batch(batch - 1)
    for group in ([b] for b in range(batch)):
        for b in group:
            wait_col(b)
        for b in group:
            finish(b)
        for b in group:
            send_power(b)

    gains.wait()
    by_gain = jnp.broadcast_to(gain[...].reshape(1, width), (CHUNK, width))

    for block in range(blocks):
        start = jnp.broadcast_to(starts[block : block + 1, :], (CHUNK, width))

        def weigh(i, carry):
            here = pl.ds(pl.multiple_of(i * CHUNK, CHUNK), CHUNK)
            there = pl.ds(pl.multiple_of(block % halves * BLOCK + i * CHUNK, CHUNK), CHUNK)
            gated = logs[block, here, :] * (local[block, here, :] + start)
            gated_ref[block // halves, there, :] = gated * by_gain
            return carry

        lax.fori_loop(0, BLOCK // CHUNK, weigh, 0, unroll=2)

    for c in range(CORES):
        several = row_buf.at[pl.ds(0, chips - c)]
        pl.when(core == c)(pltpu.make_async_copy(several, several, row_send).wait)
    pl.when(leads)(pltpu.make_async_copy(hand_buf, hand_buf, hand_send).wait)
    for k in range(1, rows):
        several = col_buf.at[pl.ds(0, k)]
        for c in range(CORES):
            copy = pltpu.make_async_copy(several, several, col_send.at[c])
            pl.when(jnp.logical_and(leads, row + k + 1 == rows))(copy.wait)
    several = power_buf.at[pl.ds(0, chans - 1)]
    pltpu.make_async_copy(several, several, power_send).wait()
    pltpu.make_async_copy(several, several, power_recv).wait()
    for b in range(batch):
        power = sum(power_buf[j, b] for j in range(chans)) * (half * half / (width * chans))
        scale_ref[b * halves : (b + 1) * halves, :] = half * lax.rsqrt(power + 1e-06)


def scale_kernel(gated_ref, scale_ref, out_hbm, result, factors, sem):
    batch, length, width = result.shape
    blocks = scale_ref.shape[0]
    halves = blocks // batch
    wide = (2 * blocks, blocks * LANES)
    pick = jnp.where(lax.rem(iota(wide, 0), blocks) == iota(wide, 1) // LANES, 1.0, 0.0).astype(BF16)
    factors[...] = lax.dot_general(
        jnp.concatenate(parts(scale_ref[...]), axis=0), pick, TN, preferred_element_type=F32
    )

    def write(block, carry):
        b, where = block // halves, lax.rem(block, halves) * BLOCK
        lane = pl.ds(pl.multiple_of(block * LANES, LANES), LANES)
        for k in range(0, BLOCK, CHUNK):
            here = pl.ds(pl.multiple_of(where + k, CHUNK), CHUNK)
            factor = jnp.concatenate([factors[k : k + CHUNK, lane]] * (width // LANES), axis=1)
            result[b, here, :] = (gated_ref[b, here, :] * factor).astype(result.dtype)
        there = (b, pl.ds(pl.multiple_of(where, BLOCK), BLOCK))
        pltpu.make_async_copy(result.at[there], out_hbm.at[there], sem).start()
        return carry

    lax.fori_loop(0, blocks, write, 0)
    pltpu.make_async_copy(result, out_hbm, sem).wait()


def solution(mesh):
    times, chans = mesh.shape["time"], mesh.shape["chan"]

    def body(decay_rate, drive_in, gate_in, norm_gain):
        batch, length, width = decay_rate.shape
        blocks = batch * length // BLOCK
        rows = times // COLS
        dma = pltpu.SemaphoreType.DMA
        vmem = pl.BlockSpec(memory_space=pltpu.VMEM)
        gated, scale = pl.pallas_call(
            functools.partial(state_kernel, times, chans),
            out_shape=(pltpu.VMEM((batch, length, width), F32), pltpu.VMEM((blocks, BLOCK), F32)),
            in_specs=[pl.BlockSpec(memory_space=pltpu.HBM)] * 4,
            out_specs=(vmem, vmem),
            scratch_shapes=[
                pltpu.VMEM((blocks, BLOCK, width), F32),
                pltpu.VMEM((blocks, 2, BLOCK, width), BF16),
                pltpu.VMEM((blocks, BLOCK, width), BF16),
                pltpu.VMEM((width,), F32),
                pltpu.VMEM((blocks, BLOCK, width), F32),
                pltpu.VMEM((blocks, BLOCK, width), F32),
                pltpu.VMEM((2, BLOCK, width), BF16),
                pltpu.VMEM((BLOCK, BLOCK), BF16),
                pltpu.VMEM((BLOCK, 2 * BLOCK), BF16),
                pltpu.VMEM((2 * blocks, width), F32),
                pltpu.VMEM((blocks, width), F32),
                pltpu.VMEM((COLS, batch, 2, width), F32),
                pltpu.VMEM((rows, batch, 2, width), F32),
                pltpu.VMEM((batch, 2, width), F32),
                pltpu.VMEM((batch, 2, width), F32),
                pltpu.VMEM((chans, batch, length // BLOCK, BLOCK), F32),
                dma((blocks + 3,)),
                dma, dma((batch,)),
                dma, dma((batch,)),
                dma((CORES,)), dma((batch,)),
                dma, dma,
            ],
            compiler_params=pltpu.CompilerParams(
                collective_id=0, has_side_effects=True, vmem_limit_bytes=57 * 2**20
            ),
        )(decay_rate, drive_in, gate_in, norm_gain)
        return pl.pallas_call(
            scale_kernel,
            out_shape=jax.ShapeDtypeStruct((batch, length, width), BF16),
            in_specs=[vmem, vmem],
            out_specs=pl.BlockSpec(memory_space=pltpu.HBM),
            scratch_shapes=[
                pltpu.VMEM((batch, length, width), BF16),
                pltpu.VMEM((BLOCK, blocks * LANES), F32),
                dma,
            ],
            compiler_params=pltpu.CompilerParams(vmem_limit_bytes=16 * 2**20),
        )(gated, scale)

    in_specs = (P(None, "time", "chan"), P(None, "time", "chan"), P(None, "time", "chan"), P("chan"))
    return jax.shard_map(body, mesh=mesh, in_specs=in_specs, out_specs=P(None, "time", "chan"), check_vma=False)
```

```python
import functools
import math

import jax
import jax.numpy as jnp
from jax import lax
from jax.experimental import pallas as pl
from jax.experimental.pallas import tpu as pltpu
from jax.sharding import PartitionSpec as P

MESH = pl.DeviceIdType.MESH
BLOCK = 256
LANES = 128
CHUNK = 16
COLS = 8
CORES = 2
F32 = jnp.float32
BF16 = jnp.bfloat16
NT = (((1,), (1,)), ((), ()))
TN = (((0,), (0,)), ((), ()))


def iota(shape, dim):
    return lax.broadcasted_iota(jnp.int32, shape, dim)


def triangle(width, value):
    row, column = iota((BLOCK, width), 0), iota((BLOCK, width), 1)
    return jnp.where(lax.rem(column, BLOCK) <= row, value, 0.0).astype(BF16)


def parts(x):
    high = x.astype(BF16)
    return high, (x - high.astype(F32)).astype(BF16)


def spread_rows(scale):
    rows = jnp.concatenate([scale, jnp.zeros((8 - scale.shape[0], BLOCK), F32)], axis=0)
    wide = (16, scale.shape[0] * LANES)
    pick = jnp.where(lax.rem(iota(wide, 0), 8) == iota(wide, 1) // LANES, 1.0, 0.0).astype(BF16)
    return lax.dot_general(jnp.concatenate(parts(rows), axis=0), pick, TN, preferred_element_type=F32)


def scale_block(part, gated, factors, store):
    width = gated.shape[-1]

    def scale_chunk(i, carry):
        here = pl.ds(pl.multiple_of(i * CHUNK, CHUNK), CHUNK)
        factor = jnp.concatenate([factors[here, part * LANES : (part + 1) * LANES]] * (width // LANES), axis=1)
        store(i, (gated[here, :] * factor).astype(BF16))
        return carry

    lax.fori_loop(0, BLOCK // CHUNK, scale_chunk, 0, unroll=4)


def state_kernel(
    times, chans, decay_hbm, drive_hbm, gate_hbm, gain_hbm, result_ref, gated_ref, scale_ref,
    decay, drives, gate, gain, logs, local, rounded, fall, lower, ends, starts, factors, row_buf, col_buf, before, hand_buf, power_buf,
    load_sem, row_send, row_recv, hand_send, hand_recv, col_send, col_recv, power_send, power_recv,
):
    batch, length, width = decay_hbm.shape
    halves = length // BLOCK
    blocks = batch * halves
    rows = times // COLS
    total_length = length * times
    log2_scale = math.log2(math.e) / total_length
    half = 0.5 * total_length**-0.5
    time, chan = lax.axis_index("time"), lax.axis_index("chan")
    row, col = time // COLS, lax.rem(time, COLS)

    def at(ref, block):
        return ref.at[block // halves, pl.ds(block % halves * BLOCK, BLOCK), :]

    def load(source, target, slot):
        return pltpu.make_async_copy(source, target, load_sem.at[slot])

    def wait_pair(slot, halves_of_pair):
        several = drives.at[pl.ds(0, halves_of_pair), 0]
        pltpu.make_async_copy(several, several, load_sem.at[slot]).wait()

    decays = [load(at(decay_hbm, k), decay.at[k], k) for k in range(blocks)]
    driving = [load(at(drive_hbm, k), drives.at[k, 0], k + 2) for k in range(blocks)]
    gates = [load(at(gate_hbm, k), gate.at[k], k // halves) for k in range(blocks)]
    gains = load(gain_hbm, gain, blocks + 2)
    decays[0].start()
    decays[1].start()
    for k in range(blocks):
        driving[k].start()
        if k + 2 < blocks:
            decays[k + 2].start()

    chips = COLS // CORES
    chip, core = col // CORES, lax.rem(col, CORES)
    leads = core == CORES - 1
    lead_of = [(row * COLS + lax.rem(chip + k, chips) * CORES + CORES - 1, chan) for k in range(chips)]
    mates = [(row * COLS + lax.rem(chip + k, chips) * CORES + c, chan) for k in range(1, chips) for c in range(CORES)]
    mate = (row * COLS + chip * CORES + CORES - 1 - core, chan)
    col_peers = [
        (lax.rem(row + k, rows) * COLS + chip * CORES + c, chan) for k in range(1, rows) for c in range(CORES)
    ]
    chan_peers = [(time, lax.rem(chan + k, chans)) for k in range(1, chans)]
    peers = mates + [mate] + col_peers + chan_peers
    barrier = pltpu.get_barrier_semaphore()
    for peer in peers:
        pl.semaphore_signal(barrier, inc=1, device_id=peer, device_id_type=MESH)

    fall[...] = triangle(BLOCK, log2_scale)
    lower[...] = triangle(2 * BLOCK, 1.0)
    chunks = [slice(k, k + CHUNK) for k in range(0, BLOCK, CHUNK)]
    none = jnp.zeros((1, width), F32)
    one = jnp.ones((1, width), F32)

    def prepare(block):
        total = jnp.zeros((8, width), F32)
        for here in chunks:
            rate = decay[block, here, :]
            total = total + (rate[:8] + rate[8:])
            rounded[block % 2, here, :] = rate.astype(BF16)
        ends[block : block + 1, :] = jnp.exp2(total.sum(0, keepdims=True) * -log2_scale)

    def mixed(block):
        total = jnp.zeros((8, width), F32)
        pieces = [(0, 256, chunks[:3]), (256, 512, chunks[3:6]), (512, width, chunks[6:])]
        for left, right, some in pieces:
            if block + 1 < blocks:
                logs[block + 1, :, left:right] = jnp.dot(
                    fall[...], rounded[(block + 1) % 2, :, left:right], preferred_element_type=F32
                )
            for here in some:
                drive, growth = drives[block, 0, here, :], jnp.exp2(logs[block, here, :])
                grown = drive.astype(F32) * growth
                total = total + (grown[:8] + grown[8:])
        ends[blocks + block : blocks + block + 1, :] = ends[block : block + 1, :] * total.sum(0, keepdims=True)

    def send_row(b):
        keep, state = one, none
        for k in range(b * halves, (b + 1) * halves):
            shrink = ends[k : k + 1, :]
            keep, state = shrink * keep, shrink * state + ends[blocks + k : blocks + k + 1, :]
        row_buf[col, b, 0:1, :] = keep
        row_buf[col, b, 1:2, :] = state

    def start_row(b):
        for k in range(1, chips):
            row_copy(b, lead_of[k]).start()
        pl.when(core == 0)(row_copy(b, lead_of[0]).start)

    def row_copy(b, peer):
        return pltpu.make_async_remote_copy(
            row_buf.at[col, b], row_buf.at[col, b], row_send, row_recv.at[b], device_id=peer, device_id_type=MESH
        )

    def handed(b):
        return pltpu.make_async_remote_copy(
            hand_buf.at[b], before.at[b], hand_send, hand_recv.at[b], device_id=mate, device_id_type=MESH
        )

    def send_col(b):
        several = row_buf.at[pl.ds(0, COLS - 1), b]
        pltpu.make_async_copy(several, several, row_recv.at[b]).wait()
        keep, state = one, none
        keep_chip, state_chip, keep_before, state_before = keep, state, keep, state
        for j in range(COLS):
            keep, state = row_buf[j, b, 0:1, :] * keep, row_buf[j, b, 0:1, :] * state + row_buf[j, b, 1:2, :]
            inside, earlier = j < col, j < chip * CORES
            keep_before, state_before = jnp.where(inside, keep, keep_before), jnp.where(inside, state, state_before)
            keep_chip, state_chip = jnp.where(earlier, keep, keep_chip), jnp.where(earlier, state, state_chip)
        col_buf[row, b, 0:1, :] = keep
        col_buf[row, b, 1:2, :] = state
        for i, peer in enumerate(col_peers):
            copy = pltpu.make_async_remote_copy(
                col_buf.at[row, b], col_buf.at[row, b], col_send.at[i % CORES], col_recv.at[b],
                device_id=peer, device_id_type=MESH,
            )
            pl.when(row + i // CORES + 1 < rows)(copy.start)
        before[b, 0:1, :] = keep_before
        before[b, 1:2, :] = state_before
        hand_buf[b, 0:1, :] = keep_chip
        hand_buf[b, 1:2, :] = state_chip
        handed(b).start()

    def wait_col(b):
        pl.when(core == 0)(handed(b).wait_recv)
        for k in range(1, rows):
            several = col_buf.at[pl.ds(0, k), b]
            pl.when(row == k)(pltpu.make_async_copy(several, several, col_recv.at[b]).wait)

    def enter(b):
        state = none
        for j in range(rows):
            state = jnp.where(j < row, col_buf[j, b, 0:1, :] * state + col_buf[j, b, 1:2, :], state)
        return before[b, 0:1, :] * state + before[b, 1:2, :]

    def gate_block(block):
        local[block] = jnp.dot(lower[...], drives[block].reshape(2 * BLOCK, width), preferred_element_type=F32)
        for here in chunks:
            opening = jnp.tanh((gate[block, here, :] * 0.5).astype(F32)) + 1.0
            logs[block, here, :] = jnp.exp2(-logs[block, here, :]) * opening

    def spread(b):
        for block in range(b * halves, (b + 1) * halves):
            for here in chunks:
                growth = jnp.exp2(logs[block, here, :]) - 1.0
                drives[block, 1, here, :] = growth.astype(BF16) * drives[block, 0, here, :]

    def gate_batch(b):
        wait_pair(b, halves)
        for block in range(b * halves, (b + 1) * halves):
            gate_block(block)
        if b + 1 < batch:
            spread(b + 1)

    def finish(b):
        start = enter(b)
        powers = jnp.zeros((halves, BLOCK), F32)
        for part in range(halves):
            block = b * halves + part
            starts[block : block + 1, :] = start
            squares = []
            for here in chunks:
                gated = logs[block, here, :] * (local[block, here, :] + start)
                square = gated * gated
                square = sum(square[:, k : k + LANES] for k in range(0, width, LANES))
                squares.append(jnp.concatenate(parts(square), axis=1))
            pick = jnp.where(iota((halves, 2 * LANES), 0) == part, 1.0, 0.0).astype(BF16)
            powers = powers + lax.dot_general(
                pick, jnp.concatenate(squares, axis=0), NT, preferred_element_type=F32
            )
            if part + 1 < halves:
                start = ends[block : block + 1, :] * (local[block, BLOCK - 1 :, :] + start)
        power_buf[chan, b] = powers

    def send_power(b):
        for peer in chan_peers:
            pltpu.make_async_remote_copy(
                power_buf.at[chan, b], power_buf.at[chan, b], power_send, power_recv.at[b],
                device_id=peer, device_id_type=MESH,
            ).start()

    decays[0].wait()
    prepare(0)
    logs[0] = jnp.dot(fall[...], rounded[0], preferred_element_type=F32)
    decays[1].wait()
    prepare(1)
    for block in range(blocks):
        wait_pair(block + 2, 3 if block + 2 < blocks else 1)
        if block == blocks // 2:
            for copy in gates[: blocks // 2]:
                copy.start()
        mixed(block)
        if block + 2 < blocks:
            prepare(block + 2)
        if block % halves == halves - 1 and block + 1 < blocks:
            b = block // halves
            send_row(b)
            if b == 1:
                pl.semaphore_wait(barrier, len(peers))
                start_row(0)
            if b >= 1:
                start_row(b)
    send_row(batch - 1)
    start_row(batch - 1)
    for copy in gates[blocks // 2 :]:
        copy.start()
    gains.start()

    spread(0)
    for b in range(batch - 1):
        gate_batch(b)
    for b in range(batch):
        pl.when(leads)(functools.partial(send_col, b))
    gate_batch(batch - 1)
    for group in ([b] for b in range(batch)):
        for b in group:
            wait_col(b)
        for b in group:
            finish(b)
        for b in group:
            send_power(b)

    gains.wait()
    by_gain = jnp.broadcast_to(gain[...].reshape(1, width), (CHUNK, width))

    for block in range(blocks):
        start = jnp.broadcast_to(starts[block : block + 1, :], (CHUNK, width))

        def weigh(i, carry):
            here = pl.ds(pl.multiple_of(i * CHUNK, CHUNK), CHUNK)
            gated = logs[block, here, :] * (local[block, here, :] + start)
            if block < blocks - halves:
                decay[block, here, :] = gated * by_gain
            else:
                gated_ref[block - blocks + halves, here, :] = gated * by_gain
            return carry

        lax.fori_loop(0, BLOCK // CHUNK, weigh, 0, unroll=2)

    for c in range(CORES):
        several = row_buf.at[pl.ds(0, chips - c)]
        pl.when(core == c)(pltpu.make_async_copy(several, several, row_send).wait)
    pl.when(leads)(pltpu.make_async_copy(hand_buf, hand_buf, hand_send).wait)
    for k in range(1, rows):
        several = col_buf.at[pl.ds(0, k)]
        for c in range(CORES):
            copy = pltpu.make_async_copy(several, several, col_send.at[c])
            pl.when(jnp.logical_and(leads, row + k + 1 == rows))(copy.wait)
    several = power_buf.at[pl.ds(0, chans - 1)]
    pltpu.make_async_copy(several, several, power_send).wait()

    def scale_of(b):
        several = power_buf.at[pl.ds(0, chans - 1), b]
        pltpu.make_async_copy(several, several, power_recv.at[b]).wait()
        power = sum(power_buf[j, b] for j in range(chans)) * (half * half / (width * chans))
        return half * lax.rsqrt(power + 1e-06)

    for b in range(batch - 1):
        factors[...] = spread_rows(scale_of(b))
        for part in range(halves):

            def store(i, value):
                where = pl.multiple_of(part * BLOCK + i * CHUNK, CHUNK)
                result_ref[b, pl.ds(where, CHUNK), :] = value

            scale_block(part, decay.at[b * halves + part], factors, store)
    scale_ref[...] = scale_of(batch - 1)


def scale_kernel(result_ref, gated_ref, scale_ref, out_hbm, last, factors, sem):
    done, halves = result_ref.shape[0], gated_ref.shape[0]

    def at(b, part):
        return b, pl.ds(part * BLOCK, BLOCK)

    for b in range(done):
        for part in range(halves):
            pltpu.make_async_copy(result_ref.at[at(b, part)], out_hbm.at[at(b, part)], sem).start()
    factors[...] = spread_rows(scale_ref[...])
    for part in range(halves):

        def store(i, value):
            where = pl.multiple_of(part * BLOCK + i * CHUNK, CHUNK)
            last[0, pl.ds(where, CHUNK), :] = value

        scale_block(part, gated_ref.at[part], factors, store)
        pltpu.make_async_copy(last.at[at(0, part)], out_hbm.at[at(done, part)], sem).start()
    pltpu.make_async_copy(out_hbm, out_hbm, sem).wait()


def solution(mesh):
    times, chans = mesh.shape["time"], mesh.shape["chan"]

    def body(decay_rate, drive_in, gate_in, norm_gain):
        batch, length, width = decay_rate.shape
        blocks = batch * length // BLOCK
        rows = times // COLS
        dma = pltpu.SemaphoreType.DMA
        vmem = pl.BlockSpec(memory_space=pltpu.VMEM)
        halves = length // BLOCK
        staged = pl.pallas_call(
            functools.partial(state_kernel, times, chans),
            out_shape=(
                pltpu.VMEM((batch - 1, length, width), BF16),
                pltpu.VMEM((halves, BLOCK, width), F32),
                pltpu.VMEM((halves, BLOCK), F32),
            ),
            in_specs=[pl.BlockSpec(memory_space=pltpu.HBM)] * 4,
            out_specs=(vmem, vmem, vmem),
            scratch_shapes=[
                pltpu.VMEM((blocks, BLOCK, width), F32),
                pltpu.VMEM((blocks, 2, BLOCK, width), BF16),
                pltpu.VMEM((blocks, BLOCK, width), BF16),
                pltpu.VMEM((width,), F32),
                pltpu.VMEM((blocks, BLOCK, width), F32),
                pltpu.VMEM((blocks, BLOCK, width), F32),
                pltpu.VMEM((2, BLOCK, width), BF16),
                pltpu.VMEM((BLOCK, BLOCK), BF16),
                pltpu.VMEM((BLOCK, 2 * BLOCK), BF16),
                pltpu.VMEM((2 * blocks, width), F32),
                pltpu.VMEM((blocks, width), F32),
                pltpu.VMEM((BLOCK, halves * LANES), F32),
                pltpu.VMEM((COLS, batch, 2, width), F32),
                pltpu.VMEM((rows, batch, 2, width), F32),
                pltpu.VMEM((batch, 2, width), F32),
                pltpu.VMEM((batch, 2, width), F32),
                pltpu.VMEM((chans, batch, length // BLOCK, BLOCK), F32),
                dma((blocks + 3,)),
                dma, dma((batch,)),
                dma, dma((batch,)),
                dma((CORES,)), dma((batch,)),
                dma, dma((batch,)),
            ],
            compiler_params=pltpu.CompilerParams(
                collective_id=0, has_side_effects=True, vmem_limit_bytes=57 * 2**20
            ),
        )(decay_rate, drive_in, gate_in, norm_gain)
        return pl.pallas_call(
            scale_kernel,
            out_shape=jax.ShapeDtypeStruct((batch, length, width), BF16),
            in_specs=[vmem, vmem, vmem],
            out_specs=pl.BlockSpec(memory_space=pltpu.HBM),
            scratch_shapes=[
                pltpu.VMEM((1, length, width), BF16),
                pltpu.VMEM((BLOCK, halves * LANES), F32),
                dma,
            ],
            compiler_params=pltpu.CompilerParams(vmem_limit_bytes=16 * 2**20),
        )(*staged)

    in_specs = (P(None, "time", "chan"), P(None, "time", "chan"), P(None, "time", "chan"), P("chan"))
    return jax.shard_map(body, mesh=mesh, in_specs=in_specs, out_specs=P(None, "time", "chan"), check_vma=False)
```

```python
import functools
import math

import jax
import jax.numpy as jnp
from jax import lax
from jax.experimental import pallas as pl
from jax.experimental.pallas import tpu as pltpu
from jax.sharding import PartitionSpec as P

MESH = pl.DeviceIdType.MESH
BLOCK = 256
LANES = 128
CHUNK = 16
COLS = 8
CORES = 2
F32 = jnp.float32
BF16 = jnp.bfloat16
NT = (((1,), (1,)), ((), ()))
TN = (((0,), (0,)), ((), ()))


def iota(shape, dim):
    return lax.broadcasted_iota(jnp.int32, shape, dim)


def triangle(width, value):
    row, column = iota((BLOCK, width), 0), iota((BLOCK, width), 1)
    return jnp.where(lax.rem(column, BLOCK) <= row, value, 0.0).astype(BF16)


def parts(x):
    high = x.astype(BF16)
    return high, (x - high.astype(F32)).astype(BF16)


def spread_rows(scale):
    rows = jnp.concatenate([scale, jnp.zeros((8 - scale.shape[0], BLOCK), F32)], axis=0)
    wide = (16, scale.shape[0] * LANES)
    pick = jnp.where(lax.rem(iota(wide, 0), 8) == iota(wide, 1) // LANES, 1.0, 0.0).astype(BF16)
    return lax.dot_general(jnp.concatenate(parts(rows), axis=0), pick, TN, preferred_element_type=F32)


def scale_block(part, gated, factors, store):
    width = gated.shape[-1]

    def scale_chunk(i, carry):
        here = pl.ds(pl.multiple_of(i * CHUNK, CHUNK), CHUNK)
        factor = jnp.concatenate([factors[here, part * LANES : (part + 1) * LANES]] * (width // LANES), axis=1)
        store(i, (gated[here, :] * factor).astype(BF16))
        return carry

    lax.fori_loop(0, BLOCK // CHUNK, scale_chunk, 0, unroll=4)


def state_kernel(
    times, chans, decay_hbm, drive_hbm, gate_hbm, gain_hbm, result_ref, gated_ref, scale_ref,
    decay, drives, gate, gain, logs, local, rounded, fall, lower, ends, starts, factors, row_buf, col_buf, before, hand_buf, power_buf,
    load_sem, row_send, row_recv, hand_send, hand_recv, col_send, col_recv, power_send, power_recv,
):
    batch, length, width = decay_hbm.shape
    halves = length // BLOCK
    blocks = batch * halves
    rows = times // COLS
    total_length = length * times
    log2_scale = math.log2(math.e) / total_length
    half = 0.5 * total_length**-0.5
    time, chan = lax.axis_index("time"), lax.axis_index("chan")
    row, col = time // COLS, lax.rem(time, COLS)

    def at(ref, block):
        return ref.at[block // halves, pl.ds(block % halves * BLOCK, BLOCK), :]

    def load(source, target, slot):
        return pltpu.make_async_copy(source, target, load_sem.at[slot])

    def wait_pair(slot, halves_of_pair):
        several = drives.at[pl.ds(0, halves_of_pair), 0]
        pltpu.make_async_copy(several, several, load_sem.at[slot]).wait()

    decays = [load(at(decay_hbm, k), decay.at[k], k) for k in range(blocks)]
    driving = [load(at(drive_hbm, k), drives.at[k, 0], k + 2) for k in range(blocks)]
    gates = [load(at(gate_hbm, k), gate.at[k], k // halves) for k in range(blocks)]
    gains = load(gain_hbm, gain, blocks + 2)
    decays[0].start()
    decays[1].start()
    for k in range(blocks):
        driving[k].start()
        if k + 2 < blocks:
            decays[k + 2].start()

    chips = COLS // CORES
    chip, core = col // CORES, lax.rem(col, CORES)
    leads = core == CORES - 1
    lead_of = [(row * COLS + lax.rem(chip + k, chips) * CORES + CORES - 1, chan) for k in range(chips)]
    mates = [(row * COLS + lax.rem(chip + k, chips) * CORES + c, chan) for k in range(1, chips) for c in range(CORES)]
    mate = (row * COLS + chip * CORES + CORES - 1 - core, chan)
    col_peers = [
        (lax.rem(row + k, rows) * COLS + chip * CORES + c, chan) for k in range(1, rows) for c in range(CORES)
    ]
    chan_peers = [(time, lax.rem(chan + k, chans)) for k in range(1, chans)]
    peers = mates + [mate] + col_peers + chan_peers
    barrier = pltpu.get_barrier_semaphore()
    for peer in peers:
        pl.semaphore_signal(barrier, inc=1, device_id=peer, device_id_type=MESH)

    fall[...] = triangle(BLOCK, log2_scale)
    lower[...] = triangle(2 * BLOCK, 1.0)
    chunks = [slice(k, k + CHUNK) for k in range(0, BLOCK, CHUNK)]
    none = jnp.zeros((1, width), F32)
    one = jnp.ones((1, width), F32)

    def prepare(block):
        total = jnp.zeros((8, width), F32)
        for here in chunks:
            rate = decay[block, here, :]
            total = total + (rate[:8] + rate[8:])
            rounded[block % 2, here, :] = rate.astype(BF16)
        ends[block : block + 1, :] = jnp.exp2(total.sum(0, keepdims=True) * -log2_scale)

    def mixed(block):
        total = jnp.zeros((8, width), F32)
        pieces = [(0, 256, chunks[:3]), (256, 512, chunks[3:6]), (512, width, chunks[6:])]
        for left, right, some in pieces:
            if block + 1 < blocks:
                logs[block + 1, :, left:right] = jnp.dot(
                    fall[...], rounded[(block + 1) % 2, :, left:right], preferred_element_type=F32
                )
            for here in some:
                drive, growth = drives[block, 0, here, :], jnp.exp2(logs[block, here, :])
                grown = drive.astype(F32) * growth
                total = total + (grown[:8] + grown[8:])
        ends[blocks + block : blocks + block + 1, :] = ends[block : block + 1, :] * total.sum(0, keepdims=True)

    def send_row(b):
        keep, state = one, none
        for k in range(b * halves, (b + 1) * halves):
            shrink = ends[k : k + 1, :]
            keep, state = shrink * keep, shrink * state + ends[blocks + k : blocks + k + 1, :]
        row_buf[col, b, 0:1, :] = keep
        row_buf[col, b, 1:2, :] = state

    def start_row(b):
        for k in range(1, chips):
            row_copy(b, lead_of[k]).start()
        pl.when(core == 0)(row_copy(b, lead_of[0]).start)

    def row_copy(b, peer):
        return pltpu.make_async_remote_copy(
            row_buf.at[col, b], row_buf.at[col, b], row_send, row_recv.at[b], device_id=peer, device_id_type=MESH
        )

    def handed(b):
        return pltpu.make_async_remote_copy(
            hand_buf.at[b], before.at[b], hand_send, hand_recv.at[b], device_id=mate, device_id_type=MESH
        )

    def send_col(b):
        several = row_buf.at[pl.ds(0, COLS - 1), b]
        pltpu.make_async_copy(several, several, row_recv.at[b]).wait()
        keep, state = one, none
        keep_chip, state_chip, keep_before, state_before = keep, state, keep, state
        for j in range(COLS):
            keep, state = row_buf[j, b, 0:1, :] * keep, row_buf[j, b, 0:1, :] * state + row_buf[j, b, 1:2, :]
            inside, earlier = j < col, j < chip * CORES
            keep_before, state_before = jnp.where(inside, keep, keep_before), jnp.where(inside, state, state_before)
            keep_chip, state_chip = jnp.where(earlier, keep, keep_chip), jnp.where(earlier, state, state_chip)
        col_buf[row, b, 0:1, :] = keep
        col_buf[row, b, 1:2, :] = state
        for i, peer in enumerate(col_peers):
            copy = pltpu.make_async_remote_copy(
                col_buf.at[row, b], col_buf.at[row, b], col_send.at[i % CORES], col_recv.at[b],
                device_id=peer, device_id_type=MESH,
            )
            pl.when(row + i // CORES + 1 < rows)(copy.start)
        before[b, 0:1, :] = keep_before
        before[b, 1:2, :] = state_before
        hand_buf[b, 0:1, :] = keep_chip
        hand_buf[b, 1:2, :] = state_chip
        handed(b).start()

    def wait_col(b):
        pl.when(core == 0)(handed(b).wait_recv)
        for k in range(1, rows):
            several = col_buf.at[pl.ds(0, k), b]
            pl.when(row == k)(pltpu.make_async_copy(several, several, col_recv.at[b]).wait)

    def enter(b):
        state = none
        for j in range(rows):
            state = jnp.where(j < row, col_buf[j, b, 0:1, :] * state + col_buf[j, b, 1:2, :], state)
        return before[b, 0:1, :] * state + before[b, 1:2, :]

    def gate_block(block):
        local[block] = jnp.dot(lower[...], drives[block].reshape(2 * BLOCK, width), preferred_element_type=F32)
        for here in chunks:
            opening = jnp.tanh((gate[block, here, :] * 0.5).astype(F32)) + 1.0
            logs[block, here, :] = jnp.exp2(-logs[block, here, :]) * opening

    def spread(b):
        for block in range(b * halves, (b + 1) * halves):
            for here in chunks:
                growth = jnp.exp2(logs[block, here, :]) - 1.0
                drives[block, 1, here, :] = growth.astype(BF16) * drives[block, 0, here, :]

    def gate_batch(b):
        wait_pair(b, halves)
        for block in range(b * halves, (b + 1) * halves):
            gate_block(block)
        if b + 1 < batch:
            spread(b + 1)

    def finish(b):
        start = enter(b)
        powers = jnp.zeros((halves, BLOCK), F32)
        for part in range(halves):
            block = b * halves + part
            starts[block : block + 1, :] = start
            squares = []
            for here in chunks:
                gated = logs[block, here, :] * (local[block, here, :] + start)
                square = gated * gated
                square = sum(square[:, k : k + LANES] for k in range(0, width, LANES))
                squares.append(jnp.concatenate(parts(square), axis=1))
            pick = jnp.where(iota((halves, 2 * LANES), 0) == part, 1.0, 0.0).astype(BF16)
            powers = powers + lax.dot_general(
                pick, jnp.concatenate(squares, axis=0), NT, preferred_element_type=F32
            )
            if part + 1 < halves:
                start = ends[block : block + 1, :] * (local[block, BLOCK - 1 :, :] + start)
        power_buf[chan, b] = powers

    def send_power(b):
        for peer in chan_peers:
            pltpu.make_async_remote_copy(
                power_buf.at[chan, b], power_buf.at[chan, b], power_send, power_recv.at[b],
                device_id=peer, device_id_type=MESH,
            ).start()

    decays[0].wait()
    prepare(0)
    logs[0] = jnp.dot(fall[...], rounded[0], preferred_element_type=F32)
    decays[1].wait()
    prepare(1)
    for block in range(blocks):
        wait_pair(block + 2, 3 if block + 2 < blocks else 1)
        if block == blocks // 2:
            for copy in gates[: blocks // 2]:
                copy.start()
        mixed(block)
        if block + 2 < blocks:
            prepare(block + 2)
        if block % halves == halves - 1 and block + 1 < blocks:
            b = block // halves
            send_row(b)
            if b == 0:
                pl.semaphore_wait(barrier, len(peers))
            start_row(b)
    send_row(batch - 1)
    start_row(batch - 1)
    for copy in gates[blocks // 2 :]:
        copy.start()
    gains.start()

    spread(0)
    for b in range(batch - 2):
        gate_batch(b)
    pl.when(leads)(functools.partial(send_col, 0))
    gate_batch(batch - 2)
    for b in range(1, batch):
        pl.when(leads)(functools.partial(send_col, b))
    gate_batch(batch - 1)
    for group in ([b] for b in range(batch)):
        for b in group:
            wait_col(b)
        for b in group:
            finish(b)
        for b in group:
            send_power(b)

    gains.wait()
    by_gain = jnp.broadcast_to(gain[...].reshape(1, width), (CHUNK, width))

    for block in range(blocks):
        start = jnp.broadcast_to(starts[block : block + 1, :], (CHUNK, width))

        def weigh(i, carry):
            here = pl.ds(pl.multiple_of(i * CHUNK, CHUNK), CHUNK)
            gated = logs[block, here, :] * (local[block, here, :] + start)
            if block < blocks - halves:
                decay[block, here, :] = gated * by_gain
            else:
                gated_ref[block - blocks + halves, here, :] = gated * by_gain
            return carry

        lax.fori_loop(0, BLOCK // CHUNK, weigh, 0, unroll=2)

    for c in range(CORES):
        several = row_buf.at[pl.ds(0, chips - c)]
        pl.when(core == c)(pltpu.make_async_copy(several, several, row_send).wait)
    pl.when(leads)(pltpu.make_async_copy(hand_buf, hand_buf, hand_send).wait)
    for k in range(1, rows):
        several = col_buf.at[pl.ds(0, k)]
        for c in range(CORES):
            copy = pltpu.make_async_copy(several, several, col_send.at[c])
            pl.when(jnp.logical_and(leads, row + k + 1 == rows))(copy.wait)
    several = power_buf.at[pl.ds(0, chans - 1)]
    pltpu.make_async_copy(several, several, power_send).wait()

    def scale_of(b):
        several = power_buf.at[pl.ds(0, chans - 1), b]
        pltpu.make_async_copy(several, several, power_recv.at[b]).wait()
        power = sum(power_buf[j, b] for j in range(chans)) * (half * half / (width * chans))
        return half * lax.rsqrt(power + 1e-06)

    for b in range(batch - 1):
        factors[...] = spread_rows(scale_of(b))
        for part in range(halves):

            def store(i, value):
                where = pl.multiple_of(part * BLOCK + i * CHUNK, CHUNK)
                result_ref[b, pl.ds(where, CHUNK), :] = value

            scale_block(part, decay.at[b * halves + part], factors, store)
    scale_ref[...] = scale_of(batch - 1)


def scale_kernel(result_ref, gated_ref, scale_ref, out_hbm, last, factors, sem):
    done, halves = result_ref.shape[0], gated_ref.shape[0]

    def at(b, part):
        return b, pl.ds(part * BLOCK, BLOCK)

    for b in range(done):
        for part in range(halves):
            pltpu.make_async_copy(result_ref.at[at(b, part)], out_hbm.at[at(b, part)], sem).start()
    factors[...] = spread_rows(scale_ref[...])
    for part in range(halves):

        def store(i, value):
            where = pl.multiple_of(part * BLOCK + i * CHUNK, CHUNK)
            last[0, pl.ds(where, CHUNK), :] = value

        scale_block(part, gated_ref.at[part], factors, store)
        pltpu.make_async_copy(last.at[at(0, part)], out_hbm.at[at(done, part)], sem).start()
    pltpu.make_async_copy(out_hbm, out_hbm, sem).wait()


def solution(mesh):
    times, chans = mesh.shape["time"], mesh.shape["chan"]

    def body(decay_rate, drive_in, gate_in, norm_gain):
        batch, length, width = decay_rate.shape
        blocks = batch * length // BLOCK
        rows = times // COLS
        dma = pltpu.SemaphoreType.DMA
        vmem = pl.BlockSpec(memory_space=pltpu.VMEM)
        halves = length // BLOCK
        staged = pl.pallas_call(
            functools.partial(state_kernel, times, chans),
            out_shape=(
                pltpu.VMEM((batch - 1, length, width), BF16),
                pltpu.VMEM((halves, BLOCK, width), F32),
                pltpu.VMEM((halves, BLOCK), F32),
            ),
            in_specs=[pl.BlockSpec(memory_space=pltpu.HBM)] * 4,
            out_specs=(vmem, vmem, vmem),
            scratch_shapes=[
                pltpu.VMEM((blocks, BLOCK, width), F32),
                pltpu.VMEM((blocks, 2, BLOCK, width), BF16),
                pltpu.VMEM((blocks, BLOCK, width), BF16),
                pltpu.VMEM((width,), F32),
                pltpu.VMEM((blocks, BLOCK, width), F32),
                pltpu.VMEM((blocks, BLOCK, width), F32),
                pltpu.VMEM((2, BLOCK, width), BF16),
                pltpu.VMEM((BLOCK, BLOCK), BF16),
                pltpu.VMEM((BLOCK, 2 * BLOCK), BF16),
                pltpu.VMEM((2 * blocks, width), F32),
                pltpu.VMEM((blocks, width), F32),
                pltpu.VMEM((BLOCK, halves * LANES), F32),
                pltpu.VMEM((COLS, batch, 2, width), F32),
                pltpu.VMEM((rows, batch, 2, width), F32),
                pltpu.VMEM((batch, 2, width), F32),
                pltpu.VMEM((batch, 2, width), F32),
                pltpu.VMEM((chans, batch, length // BLOCK, BLOCK), F32),
                dma((blocks + 3,)),
                dma, dma((batch,)),
                dma, dma((batch,)),
                dma((CORES,)), dma((batch,)),
                dma, dma((batch,)),
            ],
            compiler_params=pltpu.CompilerParams(
                collective_id=0, has_side_effects=True, vmem_limit_bytes=57 * 2**20
            ),
        )(decay_rate, drive_in, gate_in, norm_gain)
        return pl.pallas_call(
            scale_kernel,
            out_shape=jax.ShapeDtypeStruct((batch, length, width), BF16),
            in_specs=[vmem, vmem, vmem],
            out_specs=pl.BlockSpec(memory_space=pltpu.HBM),
            scratch_shapes=[
                pltpu.VMEM((1, length, width), BF16),
                pltpu.VMEM((BLOCK, halves * LANES), F32),
                dma,
            ],
            compiler_params=pltpu.CompilerParams(vmem_limit_bytes=16 * 2**20),
        )(*staged)

    in_specs = (P(None, "time", "chan"), P(None, "time", "chan"), P(None, "time", "chan"), P("chan"))
    return jax.shard_map(body, mesh=mesh, in_specs=in_specs, out_specs=P(None, "time", "chan"), check_vma=False)
```

```python
import functools
import math

import jax
import jax.numpy as jnp
from jax import lax
from jax.experimental import pallas as pl
from jax.experimental.pallas import tpu as pltpu
from jax.sharding import PartitionSpec as P

MESH = pl.DeviceIdType.MESH
BLOCK = 256
LANES = 128
CHUNK = 16
COLS = 8
CORES = 2
F32 = jnp.float32
BF16 = jnp.bfloat16
NT = (((1,), (1,)), ((), ()))
TN = (((0,), (0,)), ((), ()))


def iota(shape, dim):
    return lax.broadcasted_iota(jnp.int32, shape, dim)


def triangle(width, value):
    row, column = iota((BLOCK, width), 0), iota((BLOCK, width), 1)
    return jnp.where(lax.rem(column, BLOCK) <= row, value, 0.0).astype(BF16)


def parts(x):
    high = x.astype(BF16)
    return high, (x - high.astype(F32)).astype(BF16)


def spread_rows(scale):
    rows = jnp.concatenate([scale, jnp.zeros((8 - scale.shape[0], BLOCK), F32)], axis=0)
    wide = (16, scale.shape[0] * LANES)
    pick = jnp.where(lax.rem(iota(wide, 0), 8) == iota(wide, 1) // LANES, 1.0, 0.0).astype(BF16)
    return lax.dot_general(jnp.concatenate(parts(rows), axis=0), pick, TN, preferred_element_type=F32)


def scale_block(part, gated, factors, store):
    width = gated.shape[-1]

    def scale_chunk(i, carry):
        here = pl.ds(pl.multiple_of(i * CHUNK, CHUNK), CHUNK)
        factor = jnp.concatenate([factors[here, part * LANES : (part + 1) * LANES]] * (width // LANES), axis=1)
        store(i, (gated[here, :] * factor).astype(BF16))
        return carry

    lax.fori_loop(0, BLOCK // CHUNK, scale_chunk, 0, unroll=4)


def state_kernel(
    times, chans, decay_hbm, drive_hbm, gate_hbm, gain_hbm, result_ref, gated_ref, scale_ref,
    decay, drives, gate, gain, logs, local, rounded, fall, lower, ends, starts, factors, row_buf, col_buf, before, hand_buf, power_buf,
    load_sem, row_send, row_recv, hand_send, col_send, col_recv, power_send, power_recv,
):
    batch, length, width = decay_hbm.shape
    halves = length // BLOCK
    blocks = batch * halves
    rows = times // COLS
    total_length = length * times
    log2_scale = math.log2(math.e) / total_length
    half = 0.5 * total_length**-0.5
    time, chan = lax.axis_index("time"), lax.axis_index("chan")
    row, col = time // COLS, lax.rem(time, COLS)

    def at(ref, block):
        return ref.at[block // halves, pl.ds(block % halves * BLOCK, BLOCK), :]

    def load(source, target, slot):
        return pltpu.make_async_copy(source, target, load_sem.at[slot])

    def wait_pair(slot, halves_of_pair):
        several = drives.at[pl.ds(0, halves_of_pair), 0]
        pltpu.make_async_copy(several, several, load_sem.at[slot]).wait()

    decays = [load(at(decay_hbm, k), decay.at[k], k) for k in range(blocks)]
    driving = [load(at(drive_hbm, k), drives.at[k, 0], k + 2) for k in range(blocks)]
    gates = [load(at(gate_hbm, k), gate.at[k], k // halves) for k in range(blocks)]
    gains = load(gain_hbm, gain, blocks // 2)
    decays[0].start()
    decays[1].start()
    for k in range(blocks):
        driving[k].start()
        if k + 2 < blocks:
            decays[k + 2].start()

    chips = COLS // CORES
    chip, core = col // CORES, lax.rem(col, CORES)
    leads = core == CORES - 1
    lead_of = [(row * COLS + lax.rem(chip + k, chips) * CORES + CORES - 1, chan) for k in range(chips)]
    mates = [(row * COLS + lax.rem(chip + k, chips) * CORES + c, chan) for k in range(1, chips) for c in range(CORES)]
    mate = (row * COLS + chip * CORES + CORES - 1 - core, chan)
    col_peers = [
        (lax.rem(row + k, rows) * COLS + chip * CORES + c, chan) for k in range(1, rows) for c in range(CORES)
    ]
    chan_peers = [(time, lax.rem(chan + k, chans)) for k in sorted(range(1, chans), key=lambda k: -min(k, chans - k))]
    peers = mates + [mate] + col_peers + chan_peers
    barrier = pltpu.get_barrier_semaphore()
    for peer in peers:
        pl.semaphore_signal(barrier, inc=1, device_id=peer, device_id_type=MESH)

    fall[...] = triangle(BLOCK, log2_scale)
    lower[...] = triangle(2 * BLOCK, 1.0)
    chunks = [slice(k, k + CHUNK) for k in range(0, BLOCK, CHUNK)]
    none = jnp.zeros((1, width), F32)
    one = jnp.ones((1, width), F32)

    def prepare(block):
        total = jnp.zeros((8, width), F32)
        for here in chunks:
            rate = decay[block, here, :]
            total = total + (rate[:8] + rate[8:])
            rounded[block % 2, here, :] = rate.astype(BF16)
        ends[block : block + 1, :] = jnp.exp2(total.sum(0, keepdims=True) * -log2_scale)

    def mixed(block):
        total = jnp.zeros((8, width), F32)
        pieces = [(0, 256, chunks[:3]), (256, 512, chunks[3:6]), (512, width, chunks[6:])]
        for left, right, some in pieces:
            if block + 1 < blocks:
                logs[block + 1, :, left:right] = jnp.dot(
                    fall[...], rounded[(block + 1) % 2, :, left:right], preferred_element_type=F32
                )
            for here in some:
                drive, growth = drives[block, 0, here, :], jnp.exp2(logs[block, here, :])
                grown = drive.astype(F32) * growth
                total = total + (grown[:8] + grown[8:])
        ends[blocks + block : blocks + block + 1, :] = ends[block : block + 1, :] * total.sum(0, keepdims=True)

    def send_row(b):
        keep, state = one, none
        for k in range(b * halves, (b + 1) * halves):
            shrink = ends[k : k + 1, :]
            keep, state = shrink * keep, shrink * state + ends[blocks + k : blocks + k + 1, :]
        row_buf[col, b, 0:1, :] = keep
        row_buf[col, b, 1:2, :] = state

    def start_row(b):
        for k in range(1, chips):
            row_copy(b, lead_of[k]).start()
        pl.when(core == 0)(row_copy(b, lead_of[0]).start)

    def row_copy(b, peer):
        return pltpu.make_async_remote_copy(
            row_buf.at[col, b], row_buf.at[col, b], row_send, row_recv.at[b], device_id=peer, device_id_type=MESH
        )

    def handed(b):
        return pltpu.make_async_remote_copy(
            hand_buf.at[b], before.at[b], hand_send, col_recv.at[b], device_id=mate, device_id_type=MESH
        )

    def send_col(b):
        several = row_buf.at[pl.ds(0, COLS - 1), b]
        pltpu.make_async_copy(several, several, row_recv.at[b]).wait()
        keep, state = one, none
        keep_chip, state_chip, keep_before, state_before = keep, state, keep, state
        for j in range(COLS):
            keep, state = row_buf[j, b, 0:1, :] * keep, row_buf[j, b, 0:1, :] * state + row_buf[j, b, 1:2, :]
            inside, earlier = j < col, j < chip * CORES
            keep_before, state_before = jnp.where(inside, keep, keep_before), jnp.where(inside, state, state_before)
            keep_chip, state_chip = jnp.where(earlier, keep, keep_chip), jnp.where(earlier, state, state_chip)
        col_buf[row, b, 0:1, :] = keep
        col_buf[row, b, 1:2, :] = state
        for i, peer in enumerate(col_peers):
            copy = pltpu.make_async_remote_copy(
                col_buf.at[row, b], col_buf.at[row, b], col_send.at[i % CORES], col_recv.at[b],
                device_id=peer, device_id_type=MESH,
            )
            pl.when(row + i // CORES + 1 < rows)(copy.start)
        before[b, 0:1, :] = keep_before
        before[b, 1:2, :] = state_before
        hand_buf[b, 0:1, :] = keep_chip
        hand_buf[b, 1:2, :] = state_chip
        handed(b).start()

    def wait_col(b):
        for k in range(1, rows + 1):
            several = col_buf.at[pl.ds(0, k), b]
            copy = pltpu.make_async_copy(several, several, col_recv.at[b])
            pl.when(row + (core == 0).astype(jnp.int32) == k)(copy.wait)

    def enter(b):
        state = none
        for j in range(rows):
            state = jnp.where(j < row, col_buf[j, b, 0:1, :] * state + col_buf[j, b, 1:2, :], state)
        return before[b, 0:1, :] * state + before[b, 1:2, :]

    def gate_block(block):
        local[block] = jnp.dot(lower[...], drives[block].reshape(2 * BLOCK, width), preferred_element_type=F32)
        for here in chunks:
            opening = jnp.tanh((gate[block, here, :] * 0.5).astype(F32)) + 1.0
            logs[block, here, :] = jnp.exp2(-logs[block, here, :]) * opening

    def spread(b):
        for block in range(b * halves, (b + 1) * halves):
            for here in chunks:
                growth = jnp.exp2(logs[block, here, :]) - 1.0
                drives[block, 1, here, :] = growth.astype(BF16) * drives[block, 0, here, :]

    def gate_batch(b):
        wait_pair(b, halves)
        for block in range(b * halves, (b + 1) * halves):
            gate_block(block)
        if b + 1 < batch:
            spread(b + 1)

    def finish(b):
        start = enter(b)
        powers = jnp.zeros((halves, BLOCK), F32)
        for part in range(halves):
            block = b * halves + part
            starts[block : block + 1, :] = start
            squares = []
            for here in chunks:
                gated = logs[block, here, :] * (local[block, here, :] + start)
                square = gated * gated
                square = sum(square[:, k : k + LANES] for k in range(0, width, LANES))
                squares.append(jnp.concatenate(parts(square), axis=1))
            pick = jnp.where(iota((halves, 2 * LANES), 0) == part, 1.0, 0.0).astype(BF16)
            powers = powers + lax.dot_general(
                pick, jnp.concatenate(squares, axis=0), NT, preferred_element_type=F32
            )
            if part + 1 < halves:
                start = ends[block : block + 1, :] * (local[block, BLOCK - 1 :, :] + start)
        power_buf[chan, b] = powers

    def send_power(b):
        for peer in chan_peers:
            pltpu.make_async_remote_copy(
                power_buf.at[chan, b], power_buf.at[chan, b], power_send, power_recv.at[b],
                device_id=peer, device_id_type=MESH,
            ).start()

    decays[0].wait()
    prepare(0)
    logs[0] = jnp.dot(fall[...], rounded[0], preferred_element_type=F32)
    decays[1].wait()
    prepare(1)
    for block in range(blocks):
        wait_pair(block + 2, 3 if block + 2 < blocks else 1)
        if block == blocks // 2:
            for copy in gates[: blocks // 2]:
                copy.start()
        mixed(block)
        if block + 2 < blocks:
            prepare(block + 2)
        if block % halves == halves - 1 and block + 1 < blocks:
            b = block // halves
            send_row(b)
            if b == 1:
                pl.semaphore_wait(barrier, len(peers))
                start_row(0)
            if b >= 1:
                start_row(b)
    send_row(batch - 1)
    start_row(batch - 1)
    for copy in gates[blocks // 2 :]:
        copy.start()
    gains.start()

    spread(0)
    for b in range(batch - 1):
        gate_batch(b)
    for b in range(batch):
        pl.when(leads)(functools.partial(send_col, b))
    gate_batch(batch - 1)
    for group in ([b] for b in range(batch)):
        for b in group:
            wait_col(b)
        for b in group:
            finish(b)
        for b in group:
            send_power(b)

    gains.wait()
    by_gain = jnp.broadcast_to(gain[...].reshape(1, width), (CHUNK, width))

    for block in range(blocks):
        start = jnp.broadcast_to(starts[block : block + 1, :], (CHUNK, width))

        def weigh(i, carry):
            here = pl.ds(pl.multiple_of(i * CHUNK, CHUNK), CHUNK)
            gated = logs[block, here, :] * (local[block, here, :] + start)
            if block < blocks - halves:
                decay[block, here, :] = gated * by_gain
            else:
                gated_ref[block - blocks + halves, here, :] = gated * by_gain
            return carry

        lax.fori_loop(0, BLOCK // CHUNK, weigh, 0, unroll=2)

    for c in range(CORES):
        several = row_buf.at[pl.ds(0, chips - c)]
        pl.when(core == c)(pltpu.make_async_copy(several, several, row_send).wait)
    pl.when(leads)(pltpu.make_async_copy(hand_buf, hand_buf, hand_send).wait)
    for k in range(1, rows):
        several = col_buf.at[pl.ds(0, k)]
        for c in range(CORES):
            copy = pltpu.make_async_copy(several, several, col_send.at[c])
            pl.when(jnp.logical_and(leads, row + k + 1 == rows))(copy.wait)
    several = power_buf.at[pl.ds(0, chans - 1)]
    pltpu.make_async_copy(several, several, power_send).wait()

    def scale_of(b):
        several = power_buf.at[pl.ds(0, chans - 1), b]
        pltpu.make_async_copy(several, several, power_recv.at[b]).wait()
        power = sum(power_buf[j, b] for j in range(chans)) * (half * half / (width * chans))
        return half * lax.rsqrt(power + 1e-06)

    for b in range(batch - 1):
        factors[...] = spread_rows(scale_of(b))
        for part in range(halves):

            def store(i, value):
                where = pl.multiple_of(part * BLOCK + i * CHUNK, CHUNK)
                result_ref[b, pl.ds(where, CHUNK), :] = value

            scale_block(part, decay.at[b * halves + part], factors, store)
    scale_ref[...] = scale_of(batch - 1)


def scale_kernel(result_ref, gated_ref, scale_ref, out_hbm, last, factors, sem):
    done, halves = result_ref.shape[0], gated_ref.shape[0]

    def at(b, part):
        return b, pl.ds(part * BLOCK, BLOCK)

    for b in range(done):
        for part in range(halves):
            pltpu.make_async_copy(result_ref.at[at(b, part)], out_hbm.at[at(b, part)], sem).start()
    factors[...] = spread_rows(scale_ref[...])
    for part in range(halves):

        def store(i, value):
            where = pl.multiple_of(part * BLOCK + i * CHUNK, CHUNK)
            last[0, pl.ds(where, CHUNK), :] = value

        scale_block(part, gated_ref.at[part], factors, store)
        pltpu.make_async_copy(last.at[at(0, part)], out_hbm.at[at(done, part)], sem).start()
    pltpu.make_async_copy(out_hbm, out_hbm, sem).wait()


def solution(mesh):
    times, chans = mesh.shape["time"], mesh.shape["chan"]

    def body(decay_rate, drive_in, gate_in, norm_gain):
        batch, length, width = decay_rate.shape
        blocks = batch * length // BLOCK
        rows = times // COLS
        dma = pltpu.SemaphoreType.DMA
        vmem = pl.BlockSpec(memory_space=pltpu.VMEM)
        halves = length // BLOCK
        staged = pl.pallas_call(
            functools.partial(state_kernel, times, chans),
            out_shape=(
                pltpu.VMEM((batch - 1, length, width), BF16),
                pltpu.VMEM((halves, BLOCK, width), F32),
                pltpu.VMEM((halves, BLOCK), F32),
            ),
            in_specs=[pl.BlockSpec(memory_space=pltpu.HBM)] * 4,
            out_specs=(vmem, vmem, vmem),
            scratch_shapes=[
                pltpu.VMEM((blocks, BLOCK, width), F32),
                pltpu.VMEM((blocks, 2, BLOCK, width), BF16),
                pltpu.VMEM((blocks, BLOCK, width), BF16),
                pltpu.VMEM((width,), F32),
                pltpu.VMEM((blocks, BLOCK, width), F32),
                pltpu.VMEM((blocks, BLOCK, width), F32),
                pltpu.VMEM((2, BLOCK, width), BF16),
                pltpu.VMEM((BLOCK, BLOCK), BF16),
                pltpu.VMEM((BLOCK, 2 * BLOCK), BF16),
                pltpu.VMEM((2 * blocks, width), F32),
                pltpu.VMEM((blocks, width), F32),
                pltpu.VMEM((BLOCK, halves * LANES), F32),
                pltpu.VMEM((COLS, batch, 2, width), F32),
                pltpu.VMEM((rows, batch, 2, width), F32),
                pltpu.VMEM((batch, 2, width), F32),
                pltpu.VMEM((batch, 2, width), F32),
                pltpu.VMEM((chans, batch, length // BLOCK, BLOCK), F32),
                dma((blocks + 2,)),
                dma, dma((batch,)),
                dma,
                dma((CORES,)), dma((batch,)),
                dma, dma((batch,)),
            ],
            compiler_params=pltpu.CompilerParams(
                collective_id=0, has_side_effects=True, vmem_limit_bytes=57 * 2**20
            ),
        )(decay_rate, drive_in, gate_in, norm_gain)
        return pl.pallas_call(
            scale_kernel,
            out_shape=jax.ShapeDtypeStruct((batch, length, width), BF16),
            in_specs=[vmem, vmem, vmem],
            out_specs=pl.BlockSpec(memory_space=pltpu.HBM),
            scratch_shapes=[
                pltpu.VMEM((1, length, width), BF16),
                pltpu.VMEM((BLOCK, halves * LANES), F32),
                dma,
            ],
            compiler_params=pltpu.CompilerParams(vmem_limit_bytes=16 * 2**20),
        )(*staged)

    in_specs = (P(None, "time", "chan"), P(None, "time", "chan"), P(None, "time", "chan"), P("chan"))
    return jax.shard_map(body, mesh=mesh, in_specs=in_specs, out_specs=P(None, "time", "chan"), check_vma=False)
```

```python
import functools
import math

import jax
import jax.numpy as jnp
from jax import lax
from jax.experimental import pallas as pl
from jax.experimental.pallas import tpu as pltpu
from jax.sharding import PartitionSpec as P

MESH = pl.DeviceIdType.MESH
BLOCK = 256
LANES = 128
CHUNK = 16
COLS = 8
CORES = 2
F32 = jnp.float32
BF16 = jnp.bfloat16
NT = (((1,), (1,)), ((), ()))
TN = (((0,), (0,)), ((), ()))


def iota(shape, dim):
    return lax.broadcasted_iota(jnp.int32, shape, dim)


def triangle(width, value):
    row, column = iota((BLOCK, width), 0), iota((BLOCK, width), 1)
    return jnp.where(lax.rem(column, BLOCK) <= row, value, 0.0).astype(BF16)


def parts(x):
    high = x.astype(BF16)
    return high, (x - high.astype(F32)).astype(BF16)


def spread_rows(scale):
    rows = jnp.concatenate([scale, jnp.zeros((8 - scale.shape[0], BLOCK), F32)], axis=0)
    wide = (16, scale.shape[0] * LANES)
    pick = jnp.where(lax.rem(iota(wide, 0), 8) == iota(wide, 1) // LANES, 1.0, 0.0).astype(BF16)
    return lax.dot_general(jnp.concatenate(parts(rows), axis=0), pick, TN, preferred_element_type=F32)


def scale_block(part, gated, factors, store):
    width = gated.shape[-1]

    def scale_chunk(i, carry):
        here = pl.ds(pl.multiple_of(i * CHUNK, CHUNK), CHUNK)
        factor = jnp.concatenate([factors[here, part * LANES : (part + 1) * LANES]] * (width // LANES), axis=1)
        store(i, (gated[here, :] * factor).astype(BF16))
        return carry

    lax.fori_loop(0, BLOCK // CHUNK, scale_chunk, 0, unroll=4)


def state_kernel(
    times, chans, decay_hbm, drive_hbm, gate_hbm, gain_hbm, result_ref, gated_ref, scale_ref,
    decay, drives, gate, gain, logs, local, rounded, fall, lower, ends, starts, factors, row_buf, col_buf, before, hand_buf, power_buf,
    load_sem, row_send, row_recv, hand_send, hand_recv, col_send, col_recv, power_send, power_recv,
):
    batch, length, width = decay_hbm.shape
    halves = length // BLOCK
    blocks = batch * halves
    rows = times // COLS
    total_length = length * times
    log2_scale = math.log2(math.e) / total_length
    half = 0.5 * total_length**-0.5
    time, chan = lax.axis_index("time"), lax.axis_index("chan")
    row, col = time // COLS, lax.rem(time, COLS)

    def at(ref, block):
        return ref.at[block // halves, pl.ds(block % halves * BLOCK, BLOCK), :]

    def load(source, target, slot):
        return pltpu.make_async_copy(source, target, load_sem.at[slot])

    def wait_pair(slot, halves_of_pair):
        several = drives.at[pl.ds(0, halves_of_pair), 0]
        pltpu.make_async_copy(several, several, load_sem.at[slot]).wait()

    decays = [load(at(decay_hbm, k), decay.at[k], k) for k in range(blocks)]
    driving = [load(at(drive_hbm, k), drives.at[k, 0], k + 2) for k in range(blocks)]
    gates = [load(at(gate_hbm, k), gate.at[k], k // halves) for k in range(blocks)]
    gains = load(gain_hbm, gain, blocks + 2)
    decays[0].start()
    decays[1].start()
    for k in range(blocks):
        driving[k].start()
        if k + 2 < blocks:
            decays[k + 2].start()

    chips = COLS // CORES
    chip, core = col // CORES, lax.rem(col, CORES)
    leads = core == CORES - 1
    lead_of = [(row * COLS + lax.rem(chip + k, chips) * CORES + CORES - 1, chan) for k in range(chips)]
    mates = [(row * COLS + lax.rem(chip + k, chips) * CORES + c, chan) for k in range(1, chips) for c in range(CORES)]
    mate = (row * COLS + chip * CORES + CORES - 1 - core, chan)
    col_peers = [
        (lax.rem(row + k, rows) * COLS + chip * CORES + c, chan) for k in range(1, rows) for c in range(CORES)
    ]
    chan_peers = [(time, lax.rem(chan + k, chans)) for k in range(1, chans)]
    peers = mates + [mate] + col_peers + chan_peers
    barrier = pltpu.get_barrier_semaphore()
    for peer in peers:
        pl.semaphore_signal(barrier, inc=1, device_id=peer, device_id_type=MESH)

    fall[...] = triangle(BLOCK, log2_scale)
    lower[...] = triangle(2 * BLOCK, 1.0)
    chunks = [slice(k, k + CHUNK) for k in range(0, BLOCK, CHUNK)]
    none = jnp.zeros((1, width), F32)
    one = jnp.ones((1, width), F32)

    def prepare(block):
        total = jnp.zeros((8, width), F32)
        for here in chunks:
            rate = decay[block, here, :]
            total = total + (rate[:8] + rate[8:])
            rounded[block % 2, here, :] = rate.astype(BF16)
        ends[block : block + 1, :] = jnp.exp2(total.sum(0, keepdims=True) * -log2_scale)

    def mixed(block):
        total = jnp.zeros((8, width), F32)
        pieces = [(0, 256, chunks[:3]), (256, 512, chunks[3:6]), (512, width, chunks[6:])]
        for left, right, some in pieces:
            if block + 1 < blocks:
                logs[block + 1, :, left:right] = jnp.dot(
                    fall[...], rounded[(block + 1) % 2, :, left:right], preferred_element_type=F32
                )
            for here in some:
                drive, growth = drives[block, 0, here, :], jnp.exp2(logs[block, here, :])
                grown = drive.astype(F32) * growth
                total = total + (grown[:8] + grown[8:])
        ends[blocks + block : blocks + block + 1, :] = ends[block : block + 1, :] * total.sum(0, keepdims=True)

    def send_row(b):
        keep, state = one, none
        for k in range(b * halves, (b + 1) * halves):
            shrink = ends[k : k + 1, :]
            keep, state = shrink * keep, shrink * state + ends[blocks + k : blocks + k + 1, :]
        row_buf[col, b, 0:1, :] = keep
        row_buf[col, b, 1:2, :] = state

    def start_row(b):
        for k in range(1, chips):
            row_copy(b, lead_of[k]).start()
        pl.when(core == 0)(row_copy(b, lead_of[0]).start)

    def row_copy(b, peer):
        return pltpu.make_async_remote_copy(
            row_buf.at[col, b], row_buf.at[col, b], row_send, row_recv.at[b], device_id=peer, device_id_type=MESH
        )

    def handed(b):
        return pltpu.make_async_remote_copy(
            hand_buf.at[b], before.at[b], hand_send, hand_recv.at[b], device_id=mate, device_id_type=MESH
        )

    def send_col(b):
        several = row_buf.at[pl.ds(0, COLS - 1), b]
        pltpu.make_async_copy(several, several, row_recv.at[b]).wait()
        keep, state = one, none
        keep_chip, state_chip, keep_before, state_before = keep, state, keep, state
        for j in range(COLS):
            keep, state = row_buf[j, b, 0:1, :] * keep, row_buf[j, b, 0:1, :] * state + row_buf[j, b, 1:2, :]
            inside, earlier = j < col, j < chip * CORES
            keep_before, state_before = jnp.where(inside, keep, keep_before), jnp.where(inside, state, state_before)
            keep_chip, state_chip = jnp.where(earlier, keep, keep_chip), jnp.where(earlier, state, state_chip)
        col_buf[row, b, 0:1, :] = keep
        col_buf[row, b, 1:2, :] = state
        for i, peer in enumerate(col_peers):
            copy = pltpu.make_async_remote_copy(
                col_buf.at[row, b], col_buf.at[row, b], col_send.at[i % CORES], col_recv.at[b],
                device_id=peer, device_id_type=MESH,
            )
            pl.when(row + i // CORES + 1 < rows)(copy.start)
        before[b, 0:1, :] = keep_before
        before[b, 1:2, :] = state_before
        hand_buf[b, 0:1, :] = keep_chip
        hand_buf[b, 1:2, :] = state_chip
        handed(b).start()

    def wait_col(b):
        pl.when(core == 0)(handed(b).wait_recv)
        for k in range(1, rows):
            several = col_buf.at[pl.ds(0, k), b]
            pl.when(row == k)(pltpu.make_async_copy(several, several, col_recv.at[b]).wait)

    def enter(b):
        state = none
        for j in range(rows):
            state = jnp.where(j < row, col_buf[j, b, 0:1, :] * state + col_buf[j, b, 1:2, :], state)
        return before[b, 0:1, :] * state + before[b, 1:2, :]

    def gate_block(block):
        local[block] = jnp.dot(lower[...], drives[block].reshape(2 * BLOCK, width), preferred_element_type=F32)
        for here in chunks:
            opening = jnp.tanh((gate[block, here, :] * 0.5).astype(F32)) + 1.0
            logs[block, here, :] = jnp.exp2(-logs[block, here, :]) * opening

    def spread(b):
        for block in range(b * halves, (b + 1) * halves):
            for here in chunks:
                growth = jnp.exp2(logs[block, here, :]) - 1.0
                drives[block, 1, here, :] = growth.astype(BF16) * drives[block, 0, here, :]

    def gate_batch(b):
        wait_pair(b, halves)
        for block in range(b * halves, (b + 1) * halves):
            gate_block(block)
        if b + 1 < batch:
            spread(b + 1)

    def finish(b):
        start = enter(b)
        powers = jnp.zeros((halves, BLOCK), F32)
        for part in range(halves):
            block = b * halves + part
            starts[block : block + 1, :] = start
            squares = []
            for here in chunks:
                gated = logs[block, here, :] * (local[block, here, :] + start)
                square = gated * gated
                square = sum(square[:, k : k + LANES] for k in range(0, width, LANES))
                squares.append(jnp.concatenate(parts(square), axis=1))
            pick = jnp.where(iota((halves, 2 * LANES), 0) == part, 1.0, 0.0).astype(BF16)
            powers = powers + lax.dot_general(
                pick, jnp.concatenate(squares, axis=0), NT, preferred_element_type=F32
            )
            if part + 1 < halves:
                start = ends[block : block + 1, :] * (local[block, BLOCK - 1 :, :] + start)
        power_buf[chan, b] = powers

    def send_power(b):
        for peer in chan_peers:
            pltpu.make_async_remote_copy(
                power_buf.at[chan, b], power_buf.at[chan, b], power_send, power_recv.at[b],
                device_id=peer, device_id_type=MESH,
            ).start()

    decays[0].wait()
    prepare(0)
    logs[0] = jnp.dot(fall[...], rounded[0], preferred_element_type=F32)
    decays[1].wait()
    prepare(1)
    for block in range(blocks):
        wait_pair(block + 2, 3 if block + 2 < blocks else 1)
        mixed(block)
        if block + 2 < blocks:
            prepare(block + 2)
        if block % halves == halves - 1 and block + 1 < blocks:
            b = block // halves
            send_row(b)
            if b == 1:
                pl.semaphore_wait(barrier, len(peers))
                start_row(0)
            if b >= 1:
                start_row(b)
    send_row(batch - 1)
    start_row(batch - 1)
    for copy in gates:
        copy.start()
    gains.start()

    spread(0)
    for b in range(batch - 1):
        gate_batch(b)
    for b in range(batch):
        pl.when(leads)(functools.partial(send_col, b))
    gate_batch(batch - 1)
    for group in ([b] for b in range(batch)):
        for b in group:
            wait_col(b)
        for b in group:
            finish(b)
        for b in group:
            send_power(b)

    gains.wait()
    by_gain = jnp.broadcast_to(gain[...].reshape(1, width), (CHUNK, width))

    for block in range(blocks):
        start = jnp.broadcast_to(starts[block : block + 1, :], (CHUNK, width))

        def weigh(i, carry):
            here = pl.ds(pl.multiple_of(i * CHUNK, CHUNK), CHUNK)
            gated = logs[block, here, :] * (local[block, here, :] + start)
            if block < blocks - halves:
                decay[block, here, :] = gated * by_gain
            else:
                gated_ref[block - blocks + halves, here, :] = gated * by_gain
            return carry

        lax.fori_loop(0, BLOCK // CHUNK, weigh, 0, unroll=2)

    for c in range(CORES):
        several = row_buf.at[pl.ds(0, chips - c)]
        pl.when(core == c)(pltpu.make_async_copy(several, several, row_send).wait)
    pl.when(leads)(pltpu.make_async_copy(hand_buf, hand_buf, hand_send).wait)
    for k in range(1, rows):
        several = col_buf.at[pl.ds(0, k)]
        for c in range(CORES):
            copy = pltpu.make_async_copy(several, several, col_send.at[c])
            pl.when(jnp.logical_and(leads, row + k + 1 == rows))(copy.wait)
    several = power_buf.at[pl.ds(0, chans - 1)]
    pltpu.make_async_copy(several, several, power_send).wait()

    def scale_of(b):
        several = power_buf.at[pl.ds(0, chans - 1), b]
        pltpu.make_async_copy(several, several, power_recv.at[b]).wait()
        power = sum(power_buf[j, b] for j in range(chans)) * (half * half / (width * chans))
        return half * lax.rsqrt(power + 1e-06)

    for b in range(batch - 1):
        factors[...] = spread_rows(scale_of(b))
        for part in range(halves):

            def store(i, value):
                where = pl.multiple_of(part * BLOCK + i * CHUNK, CHUNK)
                result_ref[b, pl.ds(where, CHUNK), :] = value

            scale_block(part, decay.at[b * halves + part], factors, store)
    scale_ref[...] = scale_of(batch - 1)


def scale_kernel(result_ref, gated_ref, scale_ref, out_hbm, last, factors, sem):
    done, halves = result_ref.shape[0], gated_ref.shape[0]

    def at(b, part):
        return b, pl.ds(part * BLOCK, BLOCK)

    for b in range(done):
        for part in range(halves):
            pltpu.make_async_copy(result_ref.at[at(b, part)], out_hbm.at[at(b, part)], sem).start()
    factors[...] = spread_rows(scale_ref[...])
    for part in range(halves):

        def store(i, value):
            where = pl.multiple_of(part * BLOCK + i * CHUNK, CHUNK)
            last[0, pl.ds(where, CHUNK), :] = value

        scale_block(part, gated_ref.at[part], factors, store)
        pltpu.make_async_copy(last.at[at(0, part)], out_hbm.at[at(done, part)], sem).start()
    pltpu.make_async_copy(out_hbm, out_hbm, sem).wait()


def solution(mesh):
    times, chans = mesh.shape["time"], mesh.shape["chan"]

    def body(decay_rate, drive_in, gate_in, norm_gain):
        batch, length, width = decay_rate.shape
        blocks = batch * length // BLOCK
        rows = times // COLS
        dma = pltpu.SemaphoreType.DMA
        vmem = pl.BlockSpec(memory_space=pltpu.VMEM)
        halves = length // BLOCK
        staged = pl.pallas_call(
            functools.partial(state_kernel, times, chans),
            out_shape=(
                pltpu.VMEM((batch - 1, length, width), BF16),
                pltpu.VMEM((halves, BLOCK, width), F32),
                pltpu.VMEM((halves, BLOCK), F32),
            ),
            in_specs=[pl.BlockSpec(memory_space=pltpu.HBM)] * 4,
            out_specs=(vmem, vmem, vmem),
            scratch_shapes=[
                pltpu.VMEM((blocks, BLOCK, width), F32),
                pltpu.VMEM((blocks, 2, BLOCK, width), BF16),
                pltpu.VMEM((blocks, BLOCK, width), BF16),
                pltpu.VMEM((width,), F32),
                pltpu.VMEM((blocks, BLOCK, width), F32),
                pltpu.VMEM((blocks, BLOCK, width), F32),
                pltpu.VMEM((2, BLOCK, width), BF16),
                pltpu.VMEM((BLOCK, BLOCK), BF16),
                pltpu.VMEM((BLOCK, 2 * BLOCK), BF16),
                pltpu.VMEM((2 * blocks, width), F32),
                pltpu.VMEM((blocks, width), F32),
                pltpu.VMEM((BLOCK, halves * LANES), F32),
                pltpu.VMEM((COLS, batch, 2, width), F32),
                pltpu.VMEM((rows, batch, 2, width), F32),
                pltpu.VMEM((batch, 2, width), F32),
                pltpu.VMEM((batch, 2, width), F32),
                pltpu.VMEM((chans, batch, length // BLOCK, BLOCK), F32),
                dma((blocks + 3,)),
                dma, dma((batch,)),
                dma, dma((batch,)),
                dma((CORES,)), dma((batch,)),
                dma, dma((batch,)),
            ],
            compiler_params=pltpu.CompilerParams(
                collective_id=0, has_side_effects=True, vmem_limit_bytes=57 * 2**20
            ),
        )(decay_rate, drive_in, gate_in, norm_gain)
        return pl.pallas_call(
            scale_kernel,
            out_shape=jax.ShapeDtypeStruct((batch, length, width), BF16),
            in_specs=[vmem, vmem, vmem],
            out_specs=pl.BlockSpec(memory_space=pltpu.HBM),
            scratch_shapes=[
                pltpu.VMEM((1, length, width), BF16),
                pltpu.VMEM((BLOCK, halves * LANES), F32),
                dma,
            ],
            compiler_params=pltpu.CompilerParams(vmem_limit_bytes=16 * 2**20),
        )(*staged)

    in_specs = (P(None, "time", "chan"), P(None, "time", "chan"), P(None, "time", "chan"), P("chan"))
    return jax.shard_map(body, mesh=mesh, in_specs=in_specs, out_specs=P(None, "time", "chan"), check_vma=False)
```
